32 devices in a mesh: dp: 4 (over y, z), sp: 8 (over x, core).
Axes of the slice: x: 4, y: 2, z: 2, core: 2. Of those that a mesh axis runs over, the one named last changes fastest.
The devices are a block of a 4x4x8 slice.
Arguments:
- x_one: bfloat16 [2048, 7168], P(('dp', 'sp')), parts along dimension 0
- seg_one: int32 [2048], P(('dp', 'sp')), parts along dimension 0
- pos_one: int32 [2048], P(('dp', 'sp')), parts along dimension 0
- x_two: bfloat16 [2048, 7168], P(('dp', 'sp')), parts along dimension 0
- seg_two: int32 [2048], P(('dp', 'sp')), parts along dimension 0
- pos_two: int32 [2048], P(('dp', 'sp')), parts along dimension 0
- w_qdown: bfloat16 [7168, 1536], replicated
- gain_q: bfloat16 [1536], replicated
- w_qup: bfloat16 [1536, 12288], replicated
- w_kvdown: bfloat16 [7168, 576], replicated
- gain_kv: bfloat16 [512], replicated
- w_kvup: bfloat16 [512, 16384], replicated
- w_out: bfloat16 [8192, 7168], replicated
Outputs:
- output 1: bfloat16 [2048, 7168], P(('dp', 'sp')), parts along dimension 0
- output 2: bfloat16 [2048, 7168], P(('dp', 'sp')), parts along dimension 0
There are 4 independent parts. The reference program is written for one: setup_inputs(seed, part) draws one part's arguments, and reference() takes and returns one part's arrays. A program takes and returns all parts, laid end to end along the dimension named above; an argument that names none is the same for every part.
All inputs are finite; a program needn't handle non-finite values.
Results may differ from the reference program's by a relative error of at most 0.0139229.
Values are sent between devices in bfloat16 or wider.
A program may use at most 768 MiB of HBM per device.

```python
import jax
import jax.numpy as jnp
from jax import lax

TOKENS = 512
D_MODEL = 7168
HEADS = 64
Q_LAT = 1536
KV_LAT = 512
ROPE_DIM = 64
NOPE_DIM = 128
V_DIM = 128
PROMPTS = 2
QK_DIM = NOPE_DIM + ROPE_DIM
KV_DOWN = KV_LAT + ROPE_DIM
ROPE_BASE = 10000.0
NORM_EPS = 1e-6


def draw_layout(draw_key):
    shuffled = jax.random.permutation(draw_key, TOKENS - 1) + 1
    cut_points = jnp.sort(shuffled[:PROMPTS - 1]).astype(jnp.int32)
    tok_index = jnp.arange(TOKENS, dtype=jnp.int32)
    prompt_ids = jnp.searchsorted(cut_points, tok_index, side='right').astype(jnp.int32)
    prompt_start = jnp.concatenate([jnp.zeros((1,), jnp.int32), cut_points])
    return prompt_ids, tok_index - prompt_start[prompt_ids]


def normal_weight(draw_key, arr_shape, fan_in, scale_by):
    return (jax.random.normal(draw_key, arr_shape, jnp.float32) * scale_by * fan_in ** -0.5).astype(jnp.bfloat16)


def setup_inputs(seed: int = 0, part: int = 0) -> dict:
    part_keys = jax.random.split(jax.random.fold_in(jax.random.key(seed), part), 4)
    weight_keys = jax.random.split(jax.random.key(seed + 1), 7)
    seg_one, pos_one = draw_layout(part_keys[0])
    seg_two, pos_two = draw_layout(part_keys[1])
    return {
        'x_one': jax.random.normal(part_keys[2], (TOKENS, D_MODEL), jnp.float32).astype(jnp.bfloat16),
        'seg_one': seg_one,
        'pos_one': pos_one,
        'x_two': jax.random.normal(part_keys[3], (TOKENS, D_MODEL), jnp.float32).astype(jnp.bfloat16),
        'seg_two': seg_two,
        'pos_two': pos_two,
        'w_qdown': normal_weight(weight_keys[0], (D_MODEL, Q_LAT), D_MODEL, 1.0),
        'gain_q': jax.random.uniform(weight_keys[1], (Q_LAT,), jnp.float32, 0.5, 1.5).astype(jnp.bfloat16),
        'w_qup': normal_weight(weight_keys[2], (Q_LAT, HEADS * QK_DIM), Q_LAT, 1.0),
        'w_kvdown': normal_weight(weight_keys[3], (D_MODEL, KV_DOWN), D_MODEL, 1.0),
        'gain_kv': jax.random.uniform(weight_keys[4], (KV_LAT,), jnp.float32, 0.5, 1.5).astype(jnp.bfloat16),
        'w_kvup': normal_weight(weight_keys[5], (KV_LAT, HEADS * (NOPE_DIM + V_DIM)), KV_LAT, 1.0),
        'w_out': normal_weight(weight_keys[6], (HEADS * V_DIM, D_MODEL), HEADS * V_DIM, 2.0),
    }


def rms_scale(pre_norm, gain_vec):
    mean_sq = jnp.mean(pre_norm * pre_norm, axis=-1, keepdims=True)
    return (pre_norm * lax.rsqrt(mean_sq + NORM_EPS) * gain_vec.astype(jnp.float32)).astype(jnp.bfloat16)


def rope_tables(positions):
    half_dim = ROPE_DIM // 2
    inv_freq = ROPE_BASE ** (-jnp.arange(half_dim, dtype=jnp.float32) / half_dim)
    angles = positions.astype(jnp.float32)[..., None] * inv_freq
    return jnp.cos(angles), jnp.sin(angles)


def rope_rotate(rot_in, cos_tab, sin_tab):
    half_dim = ROPE_DIM // 2
    first_half = rot_in[..., :half_dim]
    second_half = rot_in[..., half_dim:]
    return jnp.concatenate([first_half * cos_tab - second_half * sin_tab, second_half * cos_tab + first_half * sin_tab], axis=-1)


def mla_block(tokens_in, prompt_ids, positions, w_qdown, gain_q, w_qup, w_kvdown, gain_kv, w_kvup, w_out):
    q_latent = rms_scale(jnp.dot(tokens_in, w_qdown, preferred_element_type=jnp.float32), gain_q)
    kv_raw = jnp.dot(tokens_in, w_kvdown, preferred_element_type=jnp.float32)
    kv_latent = rms_scale(kv_raw[:, :KV_LAT], gain_kv)
    cos_tab, sin_tab = rope_tables(positions)
    k_rope = rope_rotate(kv_raw[:, KV_LAT:], cos_tab, sin_tab).astype(jnp.bfloat16)
    allowed = (prompt_ids[:, None] == prompt_ids[None, :]) & (positions[None, :] <= positions[:, None])
    wq_heads = w_qup.reshape(Q_LAT, HEADS, QK_DIM).transpose(1, 0, 2)
    wkv_heads = w_kvup.reshape(KV_LAT, HEADS, NOPE_DIM + V_DIM).transpose(1, 0, 2)

    def one_head(head_weights):
        wq_head, wkv_head = head_weights
        q_head = jnp.dot(q_latent, wq_head, preferred_element_type=jnp.float32)
        q_nope = q_head[:, :NOPE_DIM].astype(jnp.bfloat16)
        q_rope = rope_rotate(q_head[:, NOPE_DIM:], cos_tab, sin_tab).astype(jnp.bfloat16)
        kv_head = jnp.dot(kv_latent, wkv_head, preferred_element_type=jnp.float32).astype(jnp.bfloat16)
        q_cat = jnp.concatenate([q_nope, q_rope], axis=1)
        k_cat = jnp.concatenate([kv_head[:, :NOPE_DIM], k_rope], axis=1)
        scores = jnp.dot(q_cat, k_cat.T, preferred_element_type=jnp.float32) * QK_DIM ** -0.5
        attn_prob = jax.nn.softmax(jnp.where(allowed, scores, -1e30), axis=-1).astype(jnp.bfloat16)
        return jnp.dot(attn_prob, kv_head[:, NOPE_DIM:], preferred_element_type=jnp.float32).astype(jnp.bfloat16)

    head_out = lax.map(one_head, (wq_heads, wkv_heads))
    attn_flat = head_out.transpose(1, 0, 2).reshape(TOKENS, HEADS * V_DIM)
    return jnp.dot(attn_flat, w_out, preferred_element_type=jnp.float32).astype(jnp.bfloat16)


def reference(x_one, seg_one, pos_one, x_two, seg_two, pos_two, w_qdown, gain_q, w_qup, w_kvdown, gain_kv, w_kvup, w_out):
    y_one = mla_block(x_one, seg_one, pos_one, w_qdown, gain_q, w_qup, w_kvdown, gain_kv, w_kvup, w_out)
    y_two = mla_block(x_two, seg_two, pos_two, w_qdown, gain_q, w_qup, w_kvdown, gain_kv, w_kvup, w_out)
    return (y_one, y_two)
```

```python
import functools

import jax
import jax.numpy as jnp
from jax import lax
from jax.experimental import pallas as pl
from jax.experimental.pallas import tpu as pltpu
from jax.sharding import PartitionSpec as P

NOPE_DIM = 128
ROPE_DIM = 64
HALF_ROPE = 32
KV_LAT = 512
Q_LAT = 1536
V_DIM = 128
QK_DIM = NOPE_DIM + ROPE_DIM
KV_DIM = NOPE_DIM + V_DIM
ROPE_BASE = 10000.0
NORM_EPS = 1e-6
LANES = 128

DOWN_ROWS = 1024
QD_SLOTS = 4
QU_HEADS = 4
QU_SLOTS = 3
KU_HEADS = 4
KU_SLOTS = 2
WO_ROWS = 2048
WO_COLS = 512
WO_SLOTS = 6
KVW = KV_LAT + LANES
MASKED = -1e30
BIG = 3e38
F32 = jnp.float32
BF16 = jnp.bfloat16


def body(n_sp, heads, d_model, blk,
         x_one, x_two, tab, w_qd, gain_q, w_qu, w_kvd, gain_kv, w_kvu, w_out,
         y_one, y_two,
         x_all, tab_all, kvd, qd, qu, ku, wo, acc_kv, acc_q, kv_all, cq_all,
         cap, kr, q_s, kvs, o_all, acc_y, y_st,
         x_sem, tab_sem, tab_ss, tab_rs, kvd_sem, qd_sem, qu_sem, ku_sem, wo_sem,
         kv_ss, kv_rs, cq_ss, cq_rs, o_ss, o_rs, y_ls, y_ss, y_rs):
    n_chip = n_sp // 2
    me = lax.axis_index("sp")
    core = lax.rem(me, 2)
    chip = me // 2
    pair = me + 1 - 2 * core
    right = lax.rem(me + 2, n_sp)
    left = lax.rem(me + n_sp - 2, n_sp)
    opp = lax.rem(me + 4, n_sp)
    q_rows = 2 * blk
    toks = n_sp * blk
    half_heads = heads // 2
    y_cols = d_model // 2
    n_down = d_model // DOWN_ROWS
    n_qu = half_heads // QU_HEADS
    n_ku = half_heads // KU_HEADS
    n_wo_k = heads * V_DIM // WO_ROWS
    n_wo_n = y_cols // WO_COLS
    n_wo = n_wo_k * n_wo_n

    def rcopy(src, dst, ss, rs, dev):
        return pltpu.make_async_remote_copy(
            src_ref=src, dst_ref=dst, send_sem=ss, recv_sem=rs,
            device_id={"sp": dev}, device_id_type=pl.DeviceIdType.MESH)

    x_in = (x_one, x_two)
    x_cp = [pltpu.make_async_copy(x_in[m], x_all.at[pl.ds(m * blk, blk)], x_sem.at[m]) for m in range(2)]
    for c in x_cp:
        c.start()

    def kvd_copy(k):
        rows = pl.ds(pl.multiple_of(k * DOWN_ROWS, DOWN_ROWS), DOWN_ROWS)
        return pltpu.make_async_copy(w_kvd.at[rows], kvd.at[rows], kvd_sem.at[k])

    def qd_copy(k):
        rows = pl.ds(pl.multiple_of(k * DOWN_ROWS, DOWN_ROWS), DOWN_ROWS)
        slot = lax.rem(k, QD_SLOTS)
        return pltpu.make_async_copy(w_qd.at[rows], qd.at[slot], qd_sem.at[slot])

    def qu_copy(i):
        width = QU_HEADS * QK_DIM
        cols = pl.ds(pl.multiple_of(core * (half_heads * QK_DIM) + i * width, LANES), width)
        slot = lax.rem(i, QU_SLOTS)
        return pltpu.make_async_copy(w_qu.at[:, cols], qu.at[slot], qu_sem.at[slot])

    def ku_copy(i):
        width = KU_HEADS * KV_DIM
        cols = pl.ds(pl.multiple_of(core * (half_heads * KV_DIM) + i * width, LANES), width)
        slot = lax.rem(i, KU_SLOTS)
        return pltpu.make_async_copy(w_kvu.at[:, cols], ku.at[slot], ku_sem.at[slot])

    def wo_copy(g):
        n = g // n_wo_k
        k = lax.rem(g, n_wo_k)
        rows = pl.ds(pl.multiple_of(k * WO_ROWS, WO_ROWS), WO_ROWS)
        cols = pl.ds(pl.multiple_of(core * y_cols + n * WO_COLS, LANES), WO_COLS)
        slot = lax.rem(g, WO_SLOTS)
        return pltpu.make_async_copy(w_out.at[rows, cols], wo.at[slot], wo_sem.at[slot])

    for k in range(n_down):
        kvd_copy(k).start()
    for k in range(QD_SLOTS):
        qd_copy(k).start()

    barrier = pltpu.get_barrier_semaphore()
    for dev in (pair, left, right):
        pl.semaphore_signal(barrier, inc=1, device_id={"sp": dev}, device_id_type=pl.DeviceIdType.MESH)
    pl.semaphore_wait(barrier, 3)

    def my_rows(m, c):
        return pl.ds(pl.multiple_of(m * q_rows + c * blk, blk), blk)

    tab_cp = [pltpu.make_async_copy(tab.at[pl.ds(m * blk, blk)], tab_all.at[my_rows(m, core)], tab_sem.at[m]) for m in range(2)]
    tab_rc = [rcopy(tab.at[pl.ds(m * blk, blk)], tab_all.at[my_rows(m, core)], tab_ss.at[m], tab_rs.at[m], pair) for m in range(2)]
    for m in range(2):
        tab_cp[m].start()
        tab_rc[m].start()
    for c in x_cp:
        c.wait()

    acc_kv[...] = jnp.zeros_like(acc_kv)

    def kv_step(k, carry):
        kvd_copy(k).wait()
        rows = pl.ds(pl.multiple_of(k * DOWN_ROWS, DOWN_ROWS), DOWN_ROWS)
        acc_kv[...] += jnp.dot(x_all[:, rows], kvd[rows, :], preferred_element_type=F32)
        return carry

    lax.fori_loop(0, n_down, kv_step, 0)
    for m in range(2):
        tab_cp[m].wait()

    lane = lax.broadcasted_iota(jnp.int32, (blk, LANES), 1)
    first_half = lax.rem(lane, ROPE_DIM) < HALF_ROPE

    def rotate(z, cos, sin, sel):
        swapped = jnp.where(sel, pltpu.roll(z, LANES - HALF_ROPE, 1), pltpu.roll(z, HALF_ROPE, 1))
        return z * cos + swapped * sin

    for m in range(2):
        rows = pl.ds(m * blk, blk)
        lat = acc_kv[rows, :KV_LAT]
        inv = lax.rsqrt(jnp.mean(lat * lat, axis=-1, keepdims=True) + NORM_EPS)
        own = pl.ds(pl.multiple_of(me * blk, blk), blk)
        kv_all[m, own, :KV_LAT] = (lat * inv * gain_kv[...].astype(F32)).astype(BF16)
        raw = acc_kv[rows, KV_LAT:]
        raw = jnp.concatenate([raw, raw], axis=1)
        t = tab_all[my_rows(m, core), :]
        kv_all[m, own, KV_LAT:] = rotate(raw, t[:, :LANES], t[:, LANES:2 * LANES], first_half).astype(BF16)

    def piece(m, dev):
        return kv_all.at[m, pl.ds(pl.multiple_of(dev * blk, blk), blk)]

    def kv_send(i, m, src_dev, role, dev):
        return rcopy(piece(m, src_dev), piece(m, src_dev), kv_ss.at[i], kv_rs.at[role, m], dev)

    def kv_wait(m, src_dev, role):
        rcopy(piece(m, src_dev), piece(m, src_dev), kv_ss.at[0], kv_rs.at[role, m], pair).wait_recv()

    sends = []
    for m in range(2):
        sends.append(kv_send(len(sends), m, me, 2, left))
        sends.append(kv_send(len(sends), m, me, 1, right))
    for m in range(2):
        sends.append(kv_send(len(sends), m, me, 0, pair))
    for c in sends:
        c.start()

    acc_q[...] = jnp.zeros_like(acc_q)

    def q_step(k, carry):
        qd_copy(k).wait()
        rows = pl.ds(pl.multiple_of(k * DOWN_ROWS, DOWN_ROWS), DOWN_ROWS)
        acc_q[...] += jnp.dot(x_all[:, rows], qd[lax.rem(k, QD_SLOTS)], preferred_element_type=F32)

        @pl.when(k + QD_SLOTS < n_down)
        def _():
            qd_copy(k + QD_SLOTS).start()

        return carry

    n_first = n_down - QD_SLOTS
    lax.fori_loop(0, n_first, q_step, 0)
    for i in range(QU_SLOTS):
        qu_copy(i).start()
    for i in range(KU_SLOTS):
        ku_copy(i).start()
    for g in range(WO_SLOTS):
        wo_copy(g).start()
    lax.fori_loop(n_first, n_down, q_step, 0)

    for m in range(2):
        rows = pl.ds(m * blk, blk)
        lat = acc_q[rows, :]
        inv = lax.rsqrt(jnp.mean(lat * lat, axis=-1, keepdims=True) + NORM_EPS)
        cq_all[my_rows(m, core), :] = (lat * inv * gain_q[...].astype(F32)).astype(BF16)
    cq_rc = [rcopy(cq_all.at[my_rows(m, core)], cq_all.at[my_rows(m, core)], cq_ss.at[m], cq_rs.at[m], pair) for m in range(2)]
    for c in cq_rc:
        c.start()

    second = []
    for m in range(2):
        kv_wait(m, left, 1)
        kv_wait(m, right, 2)
    second.append(kv_send(6, 0, left, 3, right))
    second.append(kv_send(7, 1, right, 3, left))
    for m in range(2):
        second.append(kv_send(8 + m, m, left, 4, pair))
        second.append(kv_send(10 + m, m, right, 5, pair))
    for c in second:
        c.start()
    sends += second

    for m in range(2):
        tab_rc[m].wait_recv()
    for m in range(2):
        start = tab_all[m * q_rows:(m + 1) * q_rows, 2 * LANES:]
        start = jnp.concatenate([start] * (toks // LANES), axis=1)
        key = lax.broadcasted_iota(jnp.int32, (q_rows, toks), 1)
        query = lax.broadcasted_iota(jnp.int32, (q_rows, toks), 0) + chip * q_rows
        keep = (key <= query) & (key.astype(F32) >= start)
        cap[m] = jnp.where(keep, BIG, MASKED)
    for c in cq_rc:
        c.wait_recv()

    lane2 = lax.broadcasted_iota(jnp.int32, (2 * q_rows, LANES), 1)
    low = lane2 < ROPE_DIM
    first_half2 = lax.rem(lane2, ROPE_DIM) < HALF_ROPE

    def qu_step(i, carry):
        qu_copy(i).wait()
        f = jnp.dot(cq_all[...], qu[lax.rem(i, QU_SLOTS)], preferred_element_type=F32)
        cos = tab_all[:, :LANES]
        sin = tab_all[:, LANES:2 * LANES]
        for p in range(QU_HEADS // 2):
            base = 2 * QK_DIM * p
            t0 = f[:, base:base + LANES]
            t1 = f[:, base + LANES:base + 2 * LANES]
            t2 = f[:, base + 2 * LANES:base + 3 * LANES]
            q_s[i, :, base:base + LANES] = t0.astype(BF16)
            q_s[i, :, base + LANES:base + 2 * LANES] = pltpu.roll(jnp.where(low, t2, t1), ROPE_DIM, 1).astype(BF16)
            q_s[i, :, base + 2 * LANES:base + 3 * LANES] = rotate(jnp.where(low, t1, t2), cos, sin, first_half2).astype(BF16)

        @pl.when(i + QU_SLOTS < n_qu)
        def _():
            qu_copy(i + QU_SLOTS).start()

        return carry

    lax.fori_loop(0, n_qu // 2, qu_step, 0)
    third = []
    for m in range(2):
        kv_wait(m, opp, 3)
        third.append(kv_send(12 + m, m, opp, 6, pair))
    for c in third:
        c.start()
    sends += third
    lax.fori_loop(n_qu // 2, n_qu, qu_step, 0)

    other = 1 - 2 * core
    for m in range(2):
        kv_wait(m, pair, 0)
        kv_wait(m, left + other, 4)
        kv_wait(m, right + other, 5)
        kv_wait(m, opp + other, 6)
    lane3 = lax.broadcasted_iota(jnp.int32, (toks, LANES), 1)
    for m in range(2):
        t = kv_all[m, :, KV_LAT:].astype(F32)
        kr[0, m] = jnp.where(lane3 < ROPE_DIM, t, 0.0).astype(BF16)
        kr[1, m] = jnp.where(lane3 < ROPE_DIM, 0.0, t).astype(BF16)

    exp_scale = QK_DIM ** -0.5 * 1.4426950408889634

    def o_copy(i):
        width = KU_HEADS * V_DIM
        cols = pl.ds(pl.multiple_of(core * (half_heads * V_DIM) + i * width, LANES), width)
        return rcopy(o_all.at[:, cols], o_all.at[:, cols], o_ss.at[i], o_rs.at[i], pair)

    def at_step(i, carry):
        ku_copy(i).wait()
        w = ku.at[lax.rem(i, KU_SLOTS)]
        for m in range(2):
            for r in range(toks // 256):
                kvs[m, r * 256:(r + 1) * 256, :] = jnp.dot(
                    kv_all[m, r * 256:(r + 1) * 256, :KV_LAT], w[...], preferred_element_type=F32).astype(BF16)

        @pl.when(i + KU_SLOTS < n_ku)
        def _():
            ku_copy(i + KU_SLOTS).start()

        for m in range(2):
            rows = slice(m * q_rows, (m + 1) * q_rows)
            for j in range(KU_HEADS):
                base = 2 * QK_DIM * (j // 2)
                nope = q_s[i, rows, base + LANES * (j % 2):base + LANES * (j % 2) + LANES]
                rope = q_s[i, rows, base + 2 * LANES:base + 3 * LANES]
                qc = jnp.concatenate([nope, rope], axis=1)
                kc = jnp.concatenate([kvs[m, :, KV_DIM * j:KV_DIM * j + NOPE_DIM], kr[j % 2, m]], axis=1)
                s = lax.dot_general(qc, kc, (((1,), (1,)), ((), ())), preferred_element_type=F32)
                s = jnp.minimum(s, cap[m])
                top = jnp.max(s, axis=-1, keepdims=True)
                e = jnp.exp2((s - top) * exp_scale)
                inv = 1.0 / jnp.sum(e, axis=-1, keepdims=True)
                p = (e * inv).astype(BF16)
                v = kvs[m, :, KV_DIM * j + NOPE_DIM:KV_DIM * (j + 1)]
                o = jnp.dot(p, v, preferred_element_type=F32).astype(BF16)
                col = pl.multiple_of(core * (half_heads * V_DIM) + i * (KU_HEADS * V_DIM) + j * V_DIM, LANES)
                o_all[rows, pl.ds(col, V_DIM)] = o
        o_copy(i).start()
        return carry

    lax.fori_loop(0, n_ku, at_step, 0)

    width = KU_HEADS * V_DIM
    for i in range(n_ku):
        cols = pl.ds(pl.multiple_of((1 - core) * (half_heads * V_DIM) + i * width, LANES), width)
        rcopy(o_all.at[:, cols], o_all.at[:, cols], o_ss.at[i], o_rs.at[i], pair).wait_recv()

    y_out = (y_one, y_two)

    def y_copies(n):
        slot = lax.rem(n, 2)
        cols = pl.ds(pl.multiple_of(core * y_cols + n * WO_COLS, LANES), WO_COLS)
        local = [pltpu.make_async_copy(y_st.at[slot, my_rows(m, core)], y_out[m].at[:, cols], y_ls.at[slot, m]) for m in range(2)]
        remote = [rcopy(y_st.at[slot, my_rows(m, 1 - core)], y_out[m].at[:, cols], y_ss.at[slot, m], y_rs.at[n, m], pair) for m in range(2)]
        return local, remote

    def y_wait(n):
        local, remote = y_copies(n)
        for m in range(2):
            local[m].wait()
            remote[m].wait_send()

    def wo_step(n, carry):
        for k in range(n_wo_k):
            g = n * n_wo_k + k
            wo_copy(g).wait()
            d = jnp.dot(o_all[:, k * WO_ROWS:(k + 1) * WO_ROWS], wo[lax.rem(g, WO_SLOTS)], preferred_element_type=F32)
            if k == 0:
                acc_y[...] = d
            else:
                acc_y[...] += d

            @pl.when(g + WO_SLOTS < n_wo)
            def _():
                wo_copy(g + WO_SLOTS).start()

        @pl.when(n >= 2)
        def _():
            y_wait(n - 2)

        y_st[lax.rem(n, 2)] = acc_y[...].astype(BF16)
        local, remote = y_copies(n)
        for m in range(2):
            local[m].start()
            remote[m].start()
        return carry

    lax.fori_loop(0, n_wo_n, wo_step, 0)
    y_wait(n_wo_n - 2)
    y_wait(n_wo_n - 1)
    for n in range(n_wo_n):
        cols = pl.ds(pl.multiple_of((1 - core) * y_cols + n * WO_COLS, LANES), WO_COLS)
        for m in range(2):
            rcopy(y_st.at[0, my_rows(m, core)], y_out[m].at[:, cols], y_ss.at[0, m], y_rs.at[n, m], pair).wait_recv()
    for m in range(2):
        tab_rc[m].wait_send()
        cq_rc[m].wait_send()
    for c in sends:
        c.wait_send()
    for i in range(n_ku):
        o_copy(i).wait_send()


def mla(n_sp, x_one, x_two, tab, w_qd, gain_q, w_qu, w_kvd, gain_kv, w_kvu, w_out):
    blk, d_model = x_one.shape
    heads = w_out.shape[0] // V_DIM
    toks = n_sp * blk
    q_rows = 2 * blk
    n_down = d_model // DOWN_ROWS
    n_qu = heads // 2 // QU_HEADS
    n_ku = heads // 2 // KU_HEADS
    n_wo_n = d_model // 2 // WO_COLS
    hbm = pl.BlockSpec(memory_space=pl.ANY)
    vmem = pl.BlockSpec(memory_space=pltpu.VMEM)
    dma = pltpu.SemaphoreType.DMA
    return pl.pallas_call(
        functools.partial(body, n_sp, heads, d_model, blk),
        out_shape=[jax.ShapeDtypeStruct((blk, d_model), BF16)] * 2,
        in_specs=[hbm, hbm, hbm, hbm, vmem, hbm, hbm, vmem, hbm, hbm],
        out_specs=[hbm, hbm],
        scratch_shapes=[
            pltpu.VMEM((2 * blk, d_model), BF16),
            pltpu.VMEM((2 * q_rows, 3 * LANES), F32),
            pltpu.VMEM((d_model, KV_LAT + ROPE_DIM), BF16),
            pltpu.VMEM((QD_SLOTS, DOWN_ROWS, Q_LAT), BF16),
            pltpu.VMEM((QU_SLOTS, Q_LAT, QU_HEADS * QK_DIM), BF16),
            pltpu.VMEM((KU_SLOTS, KV_LAT, KU_HEADS * KV_DIM), BF16),
            pltpu.VMEM((WO_SLOTS, WO_ROWS, WO_COLS), BF16),
            pltpu.VMEM((2 * blk, KV_LAT + ROPE_DIM), F32),
            pltpu.VMEM((2 * blk, Q_LAT), F32),
            pltpu.VMEM((2, toks, KVW), BF16),
            pltpu.VMEM((2 * q_rows, Q_LAT), BF16),
            pltpu.VMEM((2, q_rows, toks), F32),
            pltpu.VMEM((2, 2, toks, LANES), BF16),
            pltpu.VMEM((n_qu, 2 * q_rows, QU_HEADS * QK_DIM), BF16),
            pltpu.VMEM((2, toks, KU_HEADS * KV_DIM), BF16),
            pltpu.VMEM((2 * q_rows, heads * V_DIM), BF16),
            pltpu.VMEM((2 * q_rows, WO_COLS), F32),
            pltpu.VMEM((2, 2 * q_rows, WO_COLS), BF16),
            dma((2,)), dma((2,)), dma((2,)), dma((2,)),
            dma((n_down,)), dma((QD_SLOTS,)), dma((QU_SLOTS,)), dma((KU_SLOTS,)), dma((WO_SLOTS,)),
            dma((14,)), dma((7, 2)),
            dma((2,)), dma((2,)),
            dma((n_ku,)), dma((n_ku,)),
            dma((2, 2)), dma((2, 2)), dma((n_wo_n, 2)),
        ],
        compiler_params=pltpu.CompilerParams(
            collective_id=0, has_side_effects=True, vmem_limit_bytes=67043328),
        name="mla",
    )(x_one, x_two, tab, w_qd, gain_q, w_qu, w_kvd, gain_kv, w_kvu, w_out)


def solution(mesh):
    tok_spec = P(('dp', 'sp'), None)
    idx_spec = P(('dp', 'sp'))
    n_sp = mesh.shape['sp']

    def table(pos):
        blk = pos.shape[0]
        inv_freq = ROPE_BASE ** (-jnp.arange(HALF_ROPE, dtype=F32) / HALF_ROPE)
        ang = pos.astype(F32)[:, None] * inv_freq
        cos, sin = jnp.cos(ang), jnp.sin(ang)
        start = lax.axis_index('sp') * blk + jnp.arange(blk, dtype=jnp.int32) - pos
        start = jnp.broadcast_to(start.astype(F32)[:, None], (blk, LANES))
        return jnp.concatenate([cos] * 4 + [-sin, sin] * 2 + [start], axis=1)

    def local_body(x_one, seg_one, pos_one, x_two, seg_two, pos_two, w_qdown, gain_q, w_qup, w_kvdown, gain_kv, w_kvup, w_out):
        tab = jnp.concatenate([table(pos_one), table(pos_two)], axis=0)
        return mla(n_sp, x_one, x_two, tab, w_qdown, gain_q.reshape(1, -1), w_qup, w_kvdown, gain_kv.reshape(1, -1), w_kvup, w_out)

    return jax.shard_map(local_body, mesh=mesh, in_specs=(tok_spec, idx_spec, idx_spec, tok_spec, idx_spec, idx_spec) + (P(),) * 7, out_specs=(tok_spec, tok_spec), check_vma=False)
```

```python
import functools

import jax
import jax.numpy as jnp
import numpy as np
from jax import lax
from jax.experimental import pallas as pl
from jax.experimental.pallas import tpu as pltpu
from jax.sharding import PartitionSpec as P

NOPE_DIM = 128
ROPE_DIM = 64
HALF_ROPE = 32
KV_LAT = 512
Q_LAT = 1536
V_DIM = 128
QK_DIM = NOPE_DIM + ROPE_DIM
KV_DIM = NOPE_DIM + V_DIM
ROPE_BASE = 10000.0
NORM_EPS = 1e-6
LANES = 128

ROWS = 1024
COLS = 512
RING = 26
QU_HEADS = 4
QU_SLOTS = 2
KU_HEADS = 2
KU_SLOTS = 4
KVW = KV_LAT + LANES
MASKED = -1e30
BIG = 3e38
F32 = jnp.float32
BF16 = jnp.bfloat16


def body(n_sp, heads, d_model, blk,
         x_one, x_two, pos, freq, w_qd, gain_q, w_qu, w_kvd, gain_kv, w_kvu, w_out,
         y_one, y_two,
         x_all, pos_all, trig, kvd, ring, qu, ku, acc_kv, acc_q, kv_all, cq_all,
         cap, kr, q_s, kvs0, kvs1, s0, s1, p0, p1, o_all, acc_y, y_st,
         x_sem, pos_sem, pos_ss, pos_rs, kvd_sem, ring_sem, qu_sem, ku_sem,
         kv_ss, kv_rs, cq_ss, cq_rs, o_ss, o_rs, y_ls, y_ss, y_rs):
    me = lax.axis_index("sp")
    core = lax.rem(me, 2)
    chip = me // 2
    pair = me + 1 - 2 * core
    right = lax.rem(me + 2, n_sp)
    left = lax.rem(me + n_sp - 2, n_sp)
    opp = lax.rem(me + 4, n_sp)
    q_rows = 2 * blk
    toks = n_sp * blk
    half_heads = heads // 2
    y_cols = d_model // 2
    n_down = d_model // ROWS
    n_qd_c = Q_LAT // COLS
    n_qd = n_down * n_qd_c
    n_qu = half_heads // QU_HEADS
    n_ku = half_heads // KU_HEADS
    n_wo_k = heads * V_DIM // ROWS
    n_wo_n = y_cols // COLS
    n_wo = n_wo_k * n_wo_n

    def rcopy(src, dst, ss, rs, dev):
        return pltpu.make_async_remote_copy(
            src_ref=src, dst_ref=dst, send_sem=ss, recv_sem=rs,
            device_id={"sp": dev}, device_id_type=pl.DeviceIdType.MESH)

    def ds(start, size):
        return pl.ds(start if isinstance(start, int) else pl.multiple_of(start, size), size)

    def kvd_copy(k):
        return pltpu.make_async_copy(w_kvd.at[:, ds(k * ROWS, ROWS)], kvd.at[k], kvd_sem.at[k])

    def qd_copy(g):
        src = w_qd.at[ds(g // n_qd_c * ROWS, ROWS), ds(lax.rem(g, n_qd_c) * COLS, COLS)]
        return pltpu.make_async_copy(src, ring.at[g], ring_sem.at[g])

    def qu_copy(i):
        width = QU_HEADS * QK_DIM
        cols = ds(core * (half_heads * QK_DIM) + i * width, width)
        slot = lax.rem(i, QU_SLOTS)
        return pltpu.make_async_copy(w_qu.at[:, cols], qu.at[slot], qu_sem.at[slot])

    def ku_copy(i):
        width = KU_HEADS * KV_DIM
        cols = ds(core * (half_heads * KV_DIM) + i * width, width)
        slot = lax.rem(i, KU_SLOTS)
        return pltpu.make_async_copy(w_kvu.at[:, cols], ku.at[slot], ku_sem.at[slot])

    def wo_slot(g):
        return lax.rem(g + n_qd, RING)

    def wo_copy(g):
        rows = ds(lax.rem(g, n_wo_k) * ROWS, ROWS)
        cols = ds(core * y_cols + g // n_wo_k * COLS, COLS)
        return pltpu.make_async_copy(w_out.at[rows, cols], ring.at[wo_slot(g)], ring_sem.at[wo_slot(g)])

    x_in = (x_one, x_two)
    x_cp = [pltpu.make_async_copy(x_in[m], x_all.at[pl.ds(m * blk, blk)], x_sem.at[m]) for m in range(2)]
    for c in x_cp:
        c.start()
    for k in range(n_down):
        kvd_copy(k).start()
    for g in range(n_qd):
        qd_copy(g).start()

    barrier = pltpu.get_barrier_semaphore()
    for dev in (pair, left, right):
        pl.semaphore_signal(barrier, inc=1, device_id={"sp": dev}, device_id_type=pl.DeviceIdType.MESH)
    pl.semaphore_wait(barrier, 3)

    def my_rows(m, c):
        return ds(m * q_rows + c * blk, blk)

    pos_cp = [pltpu.make_async_copy(pos.at[pl.ds(m * blk, blk)], pos_all.at[my_rows(m, core)], pos_sem.at[m]) for m in range(2)]
    pos_rc = [rcopy(pos.at[pl.ds(m * blk, blk)], pos_all.at[my_rows(m, core)], pos_ss.at[m], pos_rs.at[m], pair) for m in range(2)]
    for m in range(2):
        pos_cp[m].start()
        pos_rc[m].start()

    for m in range(2):
        pos_cp[m].wait()
        pos_rc[m].wait_recv()
    lane2 = lax.broadcasted_iota(jnp.int32, (2 * q_rows, LANES), 1)
    first_half2 = lax.rem(lane2, ROPE_DIM) < HALF_ROPE
    ang = pos_all[...] * freq[...]
    trig[0] = jnp.cos(ang)
    sin = jnp.sin(ang)
    trig[1] = jnp.where(first_half2, -sin, sin)
    for m in range(2):
        row = lax.broadcasted_iota(jnp.int32, (q_rows, LANES), 0) + chip * q_rows
        start = row.astype(F32) - pos_all[m * q_rows:(m + 1) * q_rows, :]
        for c in range(toks // LANES):
            key = lax.broadcasted_iota(jnp.int32, (q_rows, LANES), 1) + c * LANES
            keep = (key <= row) & (key.astype(F32) >= start)
            cap[m, :, c * LANES:(c + 1) * LANES] = jnp.where(keep, BIG, MASKED)
    for c in x_cp:
        c.wait()

    acc_kv[...] = jnp.zeros_like(acc_kv)

    def kv_step(k, carry):
        kvd_copy(k).wait()
        acc_kv[...] += lax.dot_general(x_all[:, ds(k * ROWS, ROWS)], kvd[k], (((1,), (1,)), ((), ())), preferred_element_type=F32)
        return carry

    lax.fori_loop(0, n_down, kv_step, 0)

    lane = lax.broadcasted_iota(jnp.int32, (blk, LANES), 1)
    first_half = lax.rem(lane, ROPE_DIM) < HALF_ROPE

    def rotate(z, cos, sin, sel):
        swapped = jnp.where(sel, pltpu.roll(z, LANES - HALF_ROPE, 1), pltpu.roll(z, HALF_ROPE, 1))
        return z * cos + swapped * sin

    own = ds(me * blk, blk)
    for m in range(2):
        rows = pl.ds(m * blk, blk)
        lat = acc_kv[rows, :KV_LAT]
        inv = lax.rsqrt(jnp.mean(lat * lat, axis=-1, keepdims=True) + NORM_EPS)
        kv_all[m, own, :KV_LAT] = (lat * inv * gain_kv[...]).astype(BF16)
        raw = acc_kv[rows, KV_LAT:]
        raw = jnp.concatenate([raw, raw], axis=1)
        kv_all[m, own, KV_LAT:] = rotate(raw, trig[0, my_rows(m, core), :], trig[1, my_rows(m, core), :], first_half).astype(BF16)

    def piece(m, dev):
        return kv_all.at[m, ds(dev * blk, blk)]

    def kv_send(i, m, src_dev, role, dev):
        return rcopy(piece(m, src_dev), piece(m, src_dev), kv_ss.at[i], kv_rs.at[role, m], dev)

    def kv_wait(m, src_dev, role):
        rcopy(piece(m, src_dev), piece(m, src_dev), kv_ss.at[0], kv_rs.at[role, m], pair).wait_recv()

    sends = []
    for m in range(2):
        sends.append(kv_send(len(sends), m, me, 2, left))
        sends.append(kv_send(len(sends), m, me, 1, right))
    for m in range(2):
        sends.append(kv_send(len(sends), m, me, 0, pair))
    for c in sends:
        c.start()
    for i in range(QU_SLOTS):
        qu_copy(i).start()
    for i in range(KU_SLOTS):
        ku_copy(i).start()

    acc_q[...] = jnp.zeros_like(acc_q)

    def q_step(k, carry):
        for c in range(n_qd_c):
            qd_copy(k * n_qd_c + c).wait()
        for c in range(n_qd_c):
            cols = slice(c * COLS, (c + 1) * COLS)
            acc_q[:, cols] += jnp.dot(x_all[:, ds(k * ROWS, ROWS)], ring[k * n_qd_c + c], preferred_element_type=F32)
        return carry

    lax.fori_loop(0, n_down, q_step, 0)

    for m in range(2):
        rows = pl.ds(m * blk, blk)
        lat = acc_q[rows, :]
        inv = lax.rsqrt(jnp.mean(lat * lat, axis=-1, keepdims=True) + NORM_EPS)
        cq_all[my_rows(m, core), :] = (lat * inv * gain_q[...]).astype(BF16)
    cq_rc = [rcopy(cq_all.at[my_rows(m, core)], cq_all.at[my_rows(m, core)], cq_ss.at[m], cq_rs.at[m], pair) for m in range(2)]
    for c in cq_rc:
        c.start()

    second = []
    for m in range(2):
        kv_wait(m, left, 1)
        kv_wait(m, right, 2)
    second.append(kv_send(6, 0, left, 3, right))
    second.append(kv_send(7, 1, right, 3, left))
    for m in range(2):
        second.append(kv_send(8 + m, m, left, 4, pair))
        second.append(kv_send(10 + m, m, right, 5, pair))
    for c in second:
        c.start()
    sends += second
    for c in cq_rc:
        c.wait_recv()

    low = lane2 < ROPE_DIM

    def qu_step(i, carry):
        qu_copy(i).wait()
        f = jnp.dot(cq_all[...], qu[lax.rem(i, QU_SLOTS)], preferred_element_type=F32)
        for p in range(QU_HEADS // 2):
            base = 2 * QK_DIM * p
            t0 = f[:, base:base + LANES]
            t1 = f[:, base + LANES:base + 2 * LANES]
            t2 = f[:, base + 2 * LANES:base + 3 * LANES]
            q_s[i, :, base:base + LANES] = t0.astype(BF16)
            q_s[i, :, base + LANES:base + 2 * LANES] = pltpu.roll(jnp.where(low, t2, t1), ROPE_DIM, 1).astype(BF16)
            q_s[i, :, base + 2 * LANES:base + 3 * LANES] = rotate(jnp.where(low, t1, t2), trig[0], trig[1], first_half2).astype(BF16)

        @pl.when(i + QU_SLOTS < n_qu)
        def _():
            qu_copy(i + QU_SLOTS).start()

        return carry

    lax.fori_loop(0, n_qu // 2, qu_step, 0)
    third = []
    for m in range(2):
        kv_wait(m, opp, 3)
        third.append(kv_send(12 + m, m, opp, 6, pair))
    for c in third:
        c.start()
    sends += third
    lax.fori_loop(n_qu // 2, n_qu, qu_step, 0)
    n_early = RING - n_qd
    for g in range(n_early):
        wo_copy(g).start()

    other = 1 - 2 * core
    for m in range(2):
        kv_wait(m, pair, 0)
        kv_wait(m, left + other, 4)
        kv_wait(m, right + other, 5)
        kv_wait(m, opp + other, 6)
    lane3 = lax.broadcasted_iota(jnp.int32, (toks, LANES), 1)
    for m in range(2):
        t = kv_all[m, :, KV_LAT:].astype(F32)
        kr[0, m] = jnp.where(lane3 < ROPE_DIM, t, 0.0).astype(BF16)
        kr[1, m] = jnp.where(lane3 < ROPE_DIM, 0.0, t).astype(BF16)

    exp_scale = QK_DIM ** -0.5 * 1.4426950408889634
    kvs, s_scr, p_scr = (kvs0, kvs1), (s0, s1), (p0, p1)
    o_width = 2 * KU_HEADS * V_DIM

    def o_copy(t):
        cols = ds(core * (half_heads * V_DIM) + t * o_width, o_width)
        return rcopy(o_all.at[:, cols], o_all.at[:, cols], o_ss.at[t], o_rs.at[t], pair)

    def kv_up(b, i):
        for m in range(2):
            kvs[b][m] = jnp.dot(kv_all[m, :, :KV_LAT], ku[lax.rem(i, KU_SLOTS)], preferred_element_type=F32).astype(BF16)

    def scores(b, t):
        for m in range(2):
            rows = slice(m * q_rows, (m + 1) * q_rows)
            for j in range(KU_HEADS):
                base = 2 * QK_DIM * b
                nope = q_s[t, rows, base + LANES * j:base + LANES * (j + 1)]
                rope = q_s[t, rows, base + 2 * LANES:base + 3 * LANES]
                qc = jnp.concatenate([nope, rope], axis=1)
                kc = jnp.concatenate([kvs[b][m, :, KV_DIM * j:KV_DIM * j + NOPE_DIM], kr[j, m]], axis=1)
                s_scr[b][KU_HEADS * m + j] = lax.dot_general(qc, kc, (((1,), (1,)), ((), ())), preferred_element_type=F32)

    def softmax(b):
        step = 32
        for m in range(2):
            for j in range(KU_HEADS):
                for r in range(q_rows // step):
                    rows = slice(r * step, (r + 1) * step)
                    s = jnp.minimum(s_scr[b][KU_HEADS * m + j, rows, :], cap[m, rows, :])
                    top = jnp.max(s, axis=-1, keepdims=True)
                    e = jnp.exp2((s - top) * exp_scale)
                    inv = 1.0 / jnp.sum(e, axis=-1, keepdims=True)
                    p_scr[b][KU_HEADS * m + j, rows, :] = (e * inv).astype(BF16)

    def values(b, t):
        for m in range(2):
            rows = slice(m * q_rows, (m + 1) * q_rows)
            for j in range(KU_HEADS):
                v = kvs[b][m, :, KV_DIM * j + NOPE_DIM:KV_DIM * (j + 1)]
                o = jnp.dot(p_scr[b][KU_HEADS * m + j], v, preferred_element_type=F32).astype(BF16)
                col = pl.multiple_of(core * (half_heads * V_DIM) + t * o_width + (KU_HEADS * b + j) * V_DIM, V_DIM)
                o_all[rows, pl.ds(col, V_DIM)] = o

    ku_copy(0).wait()
    kv_up(0, 0)
    scores(0, 0)
    ku_copy(KU_SLOTS).start()
    n_loop = n_ku // 2 - 1
    n_late = RING - n_early
    per = -(-n_late // n_loop)

    def at_step(t, carry):
        ku_copy(2 * t + 1).wait()
        ku_copy(2 * t + 2).wait()
        softmax(0)
        kv_up(1, 2 * t + 1)
        values(0, t)
        scores(1, t)
        softmax(1)
        kv_up(0, 2 * t + 2)
        values(1, t)
        scores(0, t + 1)
        for d in (5, 6):
            @pl.when(2 * t + d < n_ku)
            def _():
                ku_copy(2 * t + d).start()
        for d in range(per):
            g = n_early + t * per + d

            @pl.when(g < RING)
            def _():
                wo_copy(g).start()

        o_copy(t).start()
        return carry

    lax.fori_loop(0, n_loop, at_step, 0)
    last = n_loop
    ku_copy(n_ku - 1).wait()
    softmax(0)
    kv_up(1, n_ku - 1)
    values(0, last)
    scores(1, last)
    softmax(1)
    values(1, last)
    o_copy(last).start()

    for t in range(n_loop + 1):
        cols = ds((1 - core) * (half_heads * V_DIM) + t * o_width, o_width)
        rcopy(o_all.at[:, cols], o_all.at[:, cols], o_ss.at[t], o_rs.at[t], pair).wait_recv()

    y_out = (y_one, y_two)

    def y_copies(n):
        slot = lax.rem(n, 2)
        cols = ds(core * y_cols + n * COLS, COLS)
        local = [pltpu.make_async_copy(y_st.at[slot, my_rows(m, core)], y_out[m].at[:, cols], y_ls.at[slot, m]) for m in range(2)]
        remote = [rcopy(y_st.at[slot, my_rows(m, 1 - core)], y_out[m].at[:, cols], y_ss.at[slot, m], y_rs.at[n, m], pair) for m in range(2)]
        return local, remote

    def y_wait(n):
        local, remote = y_copies(n)
        for m in range(2):
            local[m].wait()
            remote[m].wait_send()

    def wo_step(n, carry):
        for k in range(n_wo_k):
            g = n * n_wo_k + k
            wo_copy(g).wait()
            d = jnp.dot(o_all[:, k * ROWS:(k + 1) * ROWS], ring[wo_slot(g)], preferred_element_type=F32)
            if k == 0:
                acc_y[...] = d
            else:
                acc_y[...] += d

            @pl.when(g + RING < n_wo)
            def _():
                wo_copy(g + RING).start()

        @pl.when(n >= 2)
        def _():
            y_wait(n - 2)

        y_st[lax.rem(n, 2)] = acc_y[...].astype(BF16)
        local, remote = y_copies(n)
        for m in range(2):
            local[m].start()
            remote[m].start()
        return carry

    lax.fori_loop(0, n_wo_n, wo_step, 0)
    y_wait(n_wo_n - 2)
    y_wait(n_wo_n - 1)
    for n in range(n_wo_n):
        cols = ds((1 - core) * y_cols + n * COLS, COLS)
        for m in range(2):
            rcopy(y_st.at[0, my_rows(m, core)], y_out[m].at[:, cols], y_ss.at[0, m], y_rs.at[n, m], pair).wait_recv()
    for m in range(2):
        pos_rc[m].wait_send()
        cq_rc[m].wait_send()
    for c in sends:
        c.wait_send()
    for t in range(n_loop + 1):
        o_copy(t).wait_send()


def mla(n_sp, x_one, x_two, pos, freq, w_qd, gain_q, w_qu, w_kvd, gain_kv, w_kvu, w_out):
    blk, d_model = x_one.shape
    heads = w_out.shape[0] // V_DIM
    toks = n_sp * blk
    q_rows = 2 * blk
    n_down = d_model // ROWS
    n_qu = heads // 2 // QU_HEADS
    n_ku = heads // 2 // KU_HEADS
    n_wo_n = d_model // 2 // COLS
    hbm = pl.BlockSpec(memory_space=pl.ANY)
    vmem = pl.BlockSpec(memory_space=pltpu.VMEM)
    dma = pltpu.SemaphoreType.DMA
    units = 2 * KU_HEADS
    return pl.pallas_call(
        functools.partial(body, n_sp, heads, d_model, blk),
        out_shape=[jax.ShapeDtypeStruct((blk, d_model), BF16)] * 2,
        in_specs=[hbm, hbm, hbm, vmem, hbm, vmem, hbm, hbm, vmem, hbm, hbm],
        out_specs=[hbm, hbm],
        scratch_shapes=[
            pltpu.VMEM((2 * blk, d_model), BF16),
            pltpu.VMEM((2 * q_rows, LANES), F32),
            pltpu.VMEM((2, 2 * q_rows, LANES), F32),
            pltpu.VMEM((n_down, KV_LAT + ROPE_DIM, ROWS), BF16),
            pltpu.VMEM((RING, ROWS, COLS), BF16),
            pltpu.VMEM((QU_SLOTS, Q_LAT, QU_HEADS * QK_DIM), BF16),
            pltpu.VMEM((KU_SLOTS, KV_LAT, KU_HEADS * KV_DIM), BF16),
            pltpu.VMEM((2 * blk, KV_LAT + ROPE_DIM), F32),
            pltpu.VMEM((2 * blk, Q_LAT), F32),
            pltpu.VMEM((2, toks, KVW), BF16),
            pltpu.VMEM((2 * q_rows, Q_LAT), BF16),
            pltpu.VMEM((2, q_rows, toks), F32),
            pltpu.VMEM((2, 2, toks, LANES), BF16),
            pltpu.VMEM((n_qu, 2 * q_rows, QU_HEADS * QK_DIM), BF16),
            pltpu.VMEM((2, toks, KU_HEADS * KV_DIM), BF16),
            pltpu.VMEM((2, toks, KU_HEADS * KV_DIM), BF16),
            pltpu.VMEM((units, q_rows, toks), F32),
            pltpu.VMEM((units, q_rows, toks), F32),
            pltpu.VMEM((units, q_rows, toks), BF16),
            pltpu.VMEM((units, q_rows, toks), BF16),
            pltpu.VMEM((2 * q_rows, heads * V_DIM), BF16),
            pltpu.VMEM((2 * q_rows, COLS), F32),
            pltpu.VMEM((2, 2 * q_rows, COLS), BF16),
            dma((2,)), dma((2,)), dma((2,)), dma((2,)),
            dma((n_down,)), dma((RING,)), dma((QU_SLOTS,)), dma((KU_SLOTS,)),
            dma((14,)), dma((7, 2)),
            dma((2,)), dma((2,)),
            dma((n_ku // 2,)), dma((n_ku // 2,)),
            dma((2, 2)), dma((2, 2)), dma((n_wo_n, 2)),
        ],
        compiler_params=pltpu.CompilerParams(
            collective_id=0, has_side_effects=True, vmem_limit_bytes=67043328),
        name="mla",
    )(x_one, x_two, pos, freq, w_qd, gain_q, w_qu, w_kvd, gain_kv, w_kvu, w_out)


def solution(mesh):
    tok_spec = P(('dp', 'sp'), None)
    idx_spec = P(('dp', 'sp'))
    n_sp = mesh.shape['sp']
    freq = ROPE_BASE ** (-(np.arange(LANES) % HALF_ROPE).astype(np.float64) / HALF_ROPE)
    freq = freq.astype(np.float32)[None, :]

    def local_body(x_one, seg_one, pos_one, x_two, seg_two, pos_two, w_qdown, gain_q, w_qup, w_kvdown, gain_kv, w_kvup, w_out):
        pos = jnp.concatenate([pos_one, pos_two]).astype(F32)
        pos = jnp.broadcast_to(pos[:, None], (pos.shape[0], LANES))
        return mla(n_sp, x_one, x_two, pos, jnp.asarray(freq), w_qdown, gain_q.astype(F32)[None, :], w_qup, w_kvdown.T, gain_kv.astype(F32)[None, :], w_kvup, w_out)

    return jax.shard_map(local_body, mesh=mesh, in_specs=(tok_spec, idx_spec, idx_spec, tok_spec, idx_spec, idx_spec) + (P(),) * 7, out_specs=(tok_spec, tok_spec), check_vma=False)
```

```python
import functools

import jax
import jax.numpy as jnp
import numpy as np
from jax import lax
from jax.experimental import pallas as pl
from jax.experimental.pallas import tpu as pltpu
from jax.sharding import PartitionSpec as P

NOPE_DIM = 128
ROPE_DIM = 64
HALF_ROPE = 32
KV_LAT = 512
Q_LAT = 1536
V_DIM = 128
QK_DIM = NOPE_DIM + ROPE_DIM
KV_DIM = NOPE_DIM + V_DIM
ROPE_BASE = 10000.0
NORM_EPS = 1e-6
LANES = 128

ROWS = 1024
COLS = 512
RING = 25
WO_RING = 24
QU_HEADS = 4
QU_SLOTS = 3
KU_HEADS = 2
KU_SLOTS = 4
KVW = KV_LAT + LANES
MASKED = -1e30
BIG = 3e38
F32 = jnp.float32
BF16 = jnp.bfloat16


def body(n_sp, heads, d_model, blk,
         x_one, x_two, pos_one, pos_two, freq, w_qd, gain_q, w_qu, w_kvd, gain_kv, w_kvu, w_out,
         y_one, y_two,
         x_all, pos_s, ends, pos_all, trig, ring, qu, ku, acc_kv, acc_q, kv_all, cq_all,
         cap, kr, q_s, kvs0, kvs1, s0, s1, p0, p1, o_all, acc_y, y_st,
         x_sem, x_ss, x_rs, pos_sem, pos_ss, pos_rs, ring_sem, qd_sem, qu_sem, ku_sem,
         kv_ss, kv_rs, cq_ss, cq_rs, o_ss, o_rs, y_ls, y_ss, y_rs):
    me = lax.axis_index("sp")
    core = lax.rem(me, 2)
    chip = me // 2
    pair = me + 1 - 2 * core
    right = lax.rem(me + 2, n_sp)
    left = lax.rem(me + n_sp - 2, n_sp)
    opp = lax.rem(me + 4, n_sp)
    q_rows = 2 * blk
    toks = n_sp * blk
    half_heads = heads // 2
    y_cols = d_model // 2
    n_down = d_model // ROWS
    q_cols = Q_LAT // 2
    n_kvd = d_model // COLS
    n_qu = half_heads // QU_HEADS
    n_ku = half_heads // KU_HEADS
    n_wo_k = heads * V_DIM // ROWS
    n_wo_n = y_cols // COLS
    n_wo = n_wo_k * n_wo_n

    def rcopy(src, dst, ss, rs, dev):
        return pltpu.make_async_remote_copy(
            src_ref=src, dst_ref=dst, send_sem=ss, recv_sem=rs,
            device_id={"sp": dev}, device_id_type=pl.DeviceIdType.MESH)

    def ds(start, size):
        return pl.ds(start if isinstance(start, int) else pl.multiple_of(start, size), size)

    def kvd_copy(k):
        dst = ring.at[k, pl.ds(0, KV_LAT + ROPE_DIM)]
        return pltpu.make_async_copy(w_kvd.at[:, ds(k * COLS, COLS)], dst, ring_sem.at[k])

    half = COLS // 2

    def qd_refs(k):
        return ring.at[n_kvd + k], ring.at[n_kvd + n_down + k // 2, :, ds(lax.rem(k, 2) * half, half)]

    def qd_copies(k):
        col = core * q_cols
        rows = ds(k * ROWS, ROWS)
        one, two = qd_refs(k)
        return (pltpu.make_async_copy(w_qd.at[rows, pl.ds(pl.multiple_of(col, half), COLS)], one, qd_sem.at[k, 0]),
                pltpu.make_async_copy(w_qd.at[rows, pl.ds(pl.multiple_of(col + COLS, half), half)], two, qd_sem.at[k, 1]))

    def qu_copy(i):
        width = QU_HEADS * QK_DIM
        cols = ds(core * (half_heads * QK_DIM) + i * width, width)
        slot = lax.rem(i, QU_SLOTS)
        return pltpu.make_async_copy(w_qu.at[:, cols], qu.at[slot], qu_sem.at[slot])

    def ku_copy(i):
        width = KU_HEADS * KV_DIM
        cols = ds(core * (half_heads * KV_DIM) + i * width, width)
        slot = lax.rem(i, KU_SLOTS)
        return pltpu.make_async_copy(w_kvu.at[:, cols], ku.at[slot], ku_sem.at[slot])

    def wo_copy(g):
        rows = ds(lax.rem(g, n_wo_k) * ROWS, ROWS)
        cols = ds(core * y_cols + g // n_wo_k * COLS, COLS)
        slot = lax.rem(g, WO_RING)
        return pltpu.make_async_copy(w_out.at[rows, cols], ring.at[slot], ring_sem.at[slot])

    x_in = (x_one, x_two)

    def x_rows(m, c):
        return ds(c * q_rows + m * blk, blk)

    def my_rows(m, c):
        return ds(m * q_rows + c * blk, blk)

    pos_cp = [pltpu.make_async_copy((pos_one, pos_two)[m], pos_s.at[m], pos_sem.at[m]) for m in range(2)]
    x_cp = [pltpu.make_async_copy(x_in[m], x_all.at[x_rows(m, core)], x_sem.at[m]) for m in range(2)]
    for c in pos_cp + x_cp:
        c.start()
    for k in range(n_kvd):
        kvd_copy(k).start()

    barrier = pltpu.get_barrier_semaphore()
    for dev in (pair, left, right):
        pl.semaphore_signal(barrier, inc=1, device_id={"sp": dev}, device_id_type=pl.DeviceIdType.MESH)
    for c in pos_cp:
        c.wait()
    for m in range(2):
        first, final = pos_s[m, 0], pos_s[m, blk - 1]
        ends[core, 2 * m] = jnp.full((8, LANES), first, jnp.int32).astype(F32)
        ends[core, 2 * m + 1] = jnp.full((8, LANES), final, jnp.int32).astype(F32)

    lane = lax.broadcasted_iota(jnp.int32, (blk, LANES), 1)
    first_half = lax.rem(lane, ROPE_DIM) < HALF_ROPE

    def positions(m, c):
        tok = lax.broadcasted_iota(jnp.int32, (blk, LANES), 0).astype(F32)
        first = jnp.concatenate([ends[c, 2 * m]] * (blk // 8), axis=0)
        back = jnp.concatenate([ends[c, 2 * m + 1]] * (blk // 8), axis=0) - (blk - 1)
        val = jnp.where(tok + back >= 0, tok + back, tok + first)
        rows = my_rows(m, c)
        pos_all[rows, :] = val
        ang = val * freq[...]
        sin = jnp.sin(ang)
        trig[0, rows, :] = jnp.cos(ang)
        trig[1, rows, :] = jnp.where(first_half, -sin, sin)

    for m in range(2):
        positions(m, core)
    pl.semaphore_wait(barrier, 3)
    x_rc = [rcopy(x_in[m], x_all.at[x_rows(m, core)], x_ss.at[m], x_rs.at[m], pair) for m in range(2)]
    for c in x_rc:
        c.start()
    ends_rc = rcopy(ends.at[core], ends.at[core], pos_ss.at[0], pos_rs.at[0], pair)
    for c in x_cp:
        c.wait()

    acc_kv[...] = jnp.zeros_like(acc_kv)

    my_x = ds(core * q_rows, q_rows)

    def kv_step(k, carry):
        for c in qd_copies(k):
            c.start()
        for c in range(2):
            kvd_copy(2 * k + c).wait()
        x_k = x_all[my_x, ds(k * ROWS, ROWS)]
        w_k = jnp.concatenate([ring[2 * k, :KV_LAT + ROPE_DIM], ring[2 * k + 1, :KV_LAT + ROPE_DIM]], axis=1)
        acc_kv[...] += lax.dot_general(x_k, w_k, (((1,), (1,)), ((), ())), preferred_element_type=F32)
        return carry

    lax.fori_loop(0, n_down, kv_step, 0)
    ends_rc.start()

    def rotate(z, cos, sin, sel):
        swapped = jnp.where(sel, pltpu.roll(z, LANES - HALF_ROPE, 1), pltpu.roll(z, HALF_ROPE, 1))
        return z * cos + swapped * sin

    own = ds(me * blk, blk)
    for m in range(2):
        rows = pl.ds(m * blk, blk)
        lat = acc_kv[rows, :KV_LAT]
        inv = lax.rsqrt(jnp.mean(lat * lat, axis=-1, keepdims=True) + NORM_EPS)
        kv_all[m, own, :KV_LAT] = (lat * inv * gain_kv[...].astype(F32).reshape(1, -1)).astype(BF16)
        raw = acc_kv[rows, KV_LAT:]
        raw = jnp.concatenate([raw, raw], axis=1)
        kv_all[m, own, KV_LAT:] = rotate(raw, trig[0, my_rows(m, core), :], trig[1, my_rows(m, core), :], first_half).astype(BF16)

    def piece(m, dev):
        return kv_all.at[m, ds(dev * blk, blk)]

    def kv_send(i, m, src_dev, role, dev):
        return rcopy(piece(m, src_dev), piece(m, src_dev), kv_ss.at[i], kv_rs.at[role, m], dev)

    def kv_wait(m, src_dev, role):
        rcopy(piece(m, src_dev), piece(m, src_dev), kv_ss.at[0], kv_rs.at[role, m], pair).wait_recv()

    sends = []
    for m in range(2):
        sends.append(kv_send(len(sends), m, me, 2, left))
        sends.append(kv_send(len(sends), m, me, 1, right))
    for m in range(2):
        sends.append(kv_send(len(sends), m, me, 0, pair))
    for c in sends:
        c.start()
    for i in range(QU_SLOTS):
        qu_copy(i).start(priority=1)
    for i in range(KU_SLOTS):
        ku_copy(i).start(priority=1)

    for c in x_rc:
        c.wait_recv()
    my_cols = ds(core * q_cols, q_cols)
    acc_q[:, my_cols] = jnp.zeros((2 * q_rows, q_cols), F32)

    def q_step(k, carry):
        for c in qd_copies(k):
            c.wait()
        one, two = qd_refs(k)
        w_k = jnp.concatenate([one[...], two[...]], axis=1)
        acc_q[:, my_cols] += jnp.dot(x_all[:, ds(k * ROWS, ROWS)], w_k, preferred_element_type=F32)
        return carry

    lax.fori_loop(0, n_down, q_step, 0)
    cq_rc = rcopy(acc_q.at[:, my_cols], acc_q.at[:, my_cols], cq_ss.at[0], cq_rs.at[0], pair)
    cq_rc.start()

    ends_rc.wait_recv()
    for m in range(2):
        positions(m, 1 - core)
    for m in range(2):
        row = lax.broadcasted_iota(jnp.int32, (q_rows, LANES), 0) + chip * q_rows
        start = row.astype(F32) - pos_all[m * q_rows:(m + 1) * q_rows, :]
        for c in range(toks // LANES):
            key = lax.broadcasted_iota(jnp.int32, (q_rows, LANES), 1) + c * LANES
            keep = (key <= row) & (key.astype(F32) >= start)
            cap[m, :, c * LANES:(c + 1) * LANES] = jnp.where(keep, BIG, MASKED)

    cq_rc.wait_recv()
    for m in range(2):
        for c in range(2):
            lat = acc_q[c * q_rows + m * blk:c * q_rows + (m + 1) * blk, :]
            inv = lax.rsqrt(jnp.mean(lat * lat, axis=-1, keepdims=True) + NORM_EPS)
            cq_all[my_rows(m, c), :] = (lat * inv * gain_q[...].astype(F32).reshape(1, -1)).astype(BF16)

    second = []
    for m in range(2):
        kv_wait(m, left, 1)
        kv_wait(m, right, 2)
    second.append(kv_send(6, 0, left, 3, right))
    second.append(kv_send(7, 1, right, 3, left))
    for m in range(2):
        second.append(kv_send(8 + m, m, left, 4, pair))
        second.append(kv_send(10 + m, m, right, 5, pair))
    for c in second:
        c.start()
    sends += second

    lane2 = lax.broadcasted_iota(jnp.int32, (2 * q_rows, LANES), 1)
    first_half2 = lax.rem(lane2, ROPE_DIM) < HALF_ROPE
    low = lane2 < ROPE_DIM

    def qu_step(i, carry):
        qu_copy(i).wait()
        f = jnp.dot(cq_all[...], qu[lax.rem(i, QU_SLOTS)], preferred_element_type=F32)
        for p in range(QU_HEADS // 2):
            base = 2 * QK_DIM * p
            t0 = f[:, base:base + LANES]
            t1 = f[:, base + LANES:base + 2 * LANES]
            t2 = f[:, base + 2 * LANES:base + 3 * LANES]
            q_s[i, :, base:base + LANES] = t0.astype(BF16)
            q_s[i, :, base + LANES:base + 2 * LANES] = pltpu.roll(jnp.where(low, t2, t1), ROPE_DIM, 1).astype(BF16)
            q_s[i, :, base + 2 * LANES:base + 3 * LANES] = rotate(jnp.where(low, t1, t2), trig[0], trig[1], first_half2).astype(BF16)

        @pl.when(i + QU_SLOTS < n_qu)
        def _():
            qu_copy(i + QU_SLOTS).start()

        return carry

    n_before = n_qu * 3 // 4
    lax.fori_loop(0, n_before, qu_step, 0)
    third = []
    for m in range(2):
        kv_wait(m, opp, 3)
        third.append(kv_send(12 + m, m, opp, 6, pair))
    for c in third:
        c.start()
    sends += third
    lax.fori_loop(n_before, n_qu, qu_step, 0)
    n_early = n_wo_k
    for g in range(n_early):
        wo_copy(g).start(priority=1)

    other = 1 - 2 * core
    for m in range(2):
        kv_wait(m, pair, 0)
        kv_wait(m, left + other, 4)
        kv_wait(m, right + other, 5)
        kv_wait(m, opp + other, 6)
    lane3 = lax.broadcasted_iota(jnp.int32, (toks, LANES), 1)
    for m in range(2):
        t = kv_all[m, :, KV_LAT:].astype(F32)
        kr[0, m] = jnp.where(lane3 < ROPE_DIM, t, 0.0).astype(BF16)
        kr[1, m] = jnp.where(lane3 < ROPE_DIM, 0.0, t).astype(BF16)

    exp_scale = QK_DIM ** -0.5 * 1.4426950408889634
    kvs, s_scr, p_scr = (kvs0, kvs1), (s0, s1), (p0, p1)
    o_width = 2 * KU_HEADS * V_DIM

    def o_copy(t):
        cols = ds(core * (half_heads * V_DIM) + t * o_width, o_width)
        return rcopy(o_all.at[:, cols], o_all.at[:, cols], o_ss.at[t], o_rs.at[t], pair)

    def kv_up(b, i):
        for m in range(2):
            kvs[b][m] = jnp.dot(kv_all[m, :, :KV_LAT], ku[lax.rem(i, KU_SLOTS)], preferred_element_type=F32).astype(BF16)

    def scores(b, t):
        for m in range(2):
            rows = slice(m * q_rows, (m + 1) * q_rows)
            for j in range(KU_HEADS):
                base = 2 * QK_DIM * b
                nope = q_s[t, rows, base + LANES * j:base + LANES * (j + 1)]
                rope = q_s[t, rows, base + 2 * LANES:base + 3 * LANES]
                qc = jnp.concatenate([nope, rope], axis=1)
                kc = jnp.concatenate([kvs[b][m, :, KV_DIM * j:KV_DIM * j + NOPE_DIM], kr[j, m]], axis=1)
                s_scr[b][KU_HEADS * m + j] = lax.dot_general(qc, kc, (((1,), (1,)), ((), ())), preferred_element_type=F32)

    def softmax(b):
        step = 32
        for m in range(2):
            for j in range(KU_HEADS):
                for r in range(q_rows // step):
                    rows = slice(r * step, (r + 1) * step)
                    s = jnp.minimum(s_scr[b][KU_HEADS * m + j, rows, :], cap[m, rows, :])
                    top = jnp.max(s, axis=-1, keepdims=True)
                    e = jnp.exp2((s - top) * exp_scale)
                    inv = 1.0 / jnp.sum(e, axis=-1, keepdims=True)
                    p_scr[b][KU_HEADS * m + j, rows, :] = (e * inv).astype(BF16)

    def values(b, t):
        for m in range(2):
            rows = slice(m * q_rows, (m + 1) * q_rows)
            for j in range(KU_HEADS):
                v = kvs[b][m, :, KV_DIM * j + NOPE_DIM:KV_DIM * (j + 1)]
                o = jnp.dot(p_scr[b][KU_HEADS * m + j], v, preferred_element_type=F32).astype(BF16)
                col = pl.multiple_of(core * (half_heads * V_DIM) + t * o_width + (KU_HEADS * b + j) * V_DIM, V_DIM)
                o_all[rows, pl.ds(col, V_DIM)] = o

    ku_copy(0).wait()
    kv_up(0, 0)
    scores(0, 0)
    ku_copy(KU_SLOTS).start()
    n_loop = n_ku // 2 - 1
    n_late = WO_RING - n_early
    per = -(-n_late // n_loop)

    def at_step(t, carry):
        ku_copy(2 * t + 1).wait()
        ku_copy(2 * t + 2).wait()
        softmax(0)
        kv_up(1, 2 * t + 1)
        values(0, t)
        scores(1, t)
        softmax(1)
        kv_up(0, 2 * t + 2)
        values(1, t)
        scores(0, t + 1)
        for d in (5, 6):
            @pl.when(2 * t + d < n_ku)
            def _():
                ku_copy(2 * t + d).start()
        for d in range(per):
            g = n_early + t * per + d

            @pl.when(g < WO_RING)
            def _():
                wo_copy(g).start(priority=1)

        o_copy(t).start()
        return carry

    lax.fori_loop(0, n_loop, at_step, 0)
    last = n_loop
    ku_copy(n_ku - 1).wait()
    softmax(0)
    kv_up(1, n_ku - 1)
    values(0, last)
    scores(1, last)
    softmax(1)
    values(1, last)
    o_copy(last).start()

    for t in range(n_loop + 1):
        cols = ds((1 - core) * (half_heads * V_DIM) + t * o_width, o_width)
        rcopy(o_all.at[:, cols], o_all.at[:, cols], o_ss.at[t], o_rs.at[t], pair).wait_recv()

    y_out = (y_one, y_two)

    def y_copies(n):
        slot = lax.rem(n, 2)
        cols = ds(core * y_cols + n * COLS, COLS)
        local = [pltpu.make_async_copy(y_st.at[slot, my_rows(m, core)], y_out[m].at[:, cols], y_ls.at[slot, m]) for m in range(2)]
        remote = [rcopy(y_st.at[slot, my_rows(m, 1 - core)], y_out[m].at[:, cols], y_ss.at[slot, m], y_rs.at[n, m], pair) for m in range(2)]
        return local, remote

    def y_wait(n):
        local, remote = y_copies(n)
        for m in range(2):
            local[m].wait()
            remote[m].wait_send()

    def wo_step(n, carry):
        for k in range(n_wo_k):
            wo_copy(n * n_wo_k + k).wait()
        first = lax.rem(n * n_wo_k, WO_RING)
        w_n = ring[pl.ds(first, n_wo_k)].reshape(n_wo_k * ROWS, COLS)
        acc_y[...] = jnp.dot(o_all[...], w_n, preferred_element_type=F32)

        @pl.when((n + 1) * n_wo_k + WO_RING <= n_wo)
        def _():
            for k in range(n_wo_k):
                wo_copy(n * n_wo_k + WO_RING + k).start()

        @pl.when(n >= 2)
        def _():
            y_wait(n - 2)

        y_st[lax.rem(n, 2)] = acc_y[...].astype(BF16)
        local, remote = y_copies(n)
        for m in range(2):
            local[m].start()
            remote[m].start()
        return carry

    lax.fori_loop(0, n_wo_n, wo_step, 0)
    y_wait(n_wo_n - 2)
    y_wait(n_wo_n - 1)
    for n in range(n_wo_n):
        cols = ds((1 - core) * y_cols + n * COLS, COLS)
        for m in range(2):
            rcopy(y_st.at[0, my_rows(m, core)], y_out[m].at[:, cols], y_ss.at[0, m], y_rs.at[n, m], pair).wait_recv()
    for c in x_rc + [ends_rc, cq_rc]:
        c.wait_send()
    for c in sends:
        c.wait_send()
    for t in range(n_loop + 1):
        o_copy(t).wait_send()


def mla(n_sp, x_one, x_two, pos_one, pos_two, freq, w_qd, gain_q, w_qu, w_kvd, gain_kv, w_kvu, w_out):
    blk, d_model = x_one.shape
    heads = w_out.shape[0] // V_DIM
    toks = n_sp * blk
    q_rows = 2 * blk
    n_down = d_model // ROWS
    n_qu = heads // 2 // QU_HEADS
    n_ku = heads // 2 // KU_HEADS
    n_wo_n = d_model // 2 // COLS
    hbm = pl.BlockSpec(memory_space=pl.ANY)
    vmem = pl.BlockSpec(memory_space=pltpu.VMEM)
    dma = pltpu.SemaphoreType.DMA
    units = 2 * KU_HEADS
    return pl.pallas_call(
        functools.partial(body, n_sp, heads, d_model, blk),
        out_shape=[jax.ShapeDtypeStruct((blk, d_model), BF16)] * 2,
        in_specs=[hbm, hbm, hbm, hbm, vmem, hbm, vmem, hbm, hbm, vmem, hbm, hbm],
        out_specs=[hbm, hbm],
        scratch_shapes=[
            pltpu.VMEM((2 * q_rows, d_model), BF16),
            pltpu.SMEM((2, blk), jnp.int32),
            pltpu.VMEM((2, 4, 8, LANES), F32),
            pltpu.VMEM((2 * q_rows, LANES), F32),
            pltpu.VMEM((2, 2 * q_rows, LANES), F32),
            pltpu.VMEM((RING, ROWS, COLS), BF16),
            pltpu.VMEM((QU_SLOTS, Q_LAT, QU_HEADS * QK_DIM), BF16),
            pltpu.VMEM((KU_SLOTS, KV_LAT, KU_HEADS * KV_DIM), BF16),
            pltpu.VMEM((2 * blk, KV_LAT + ROPE_DIM), F32),
            pltpu.VMEM((2 * q_rows, Q_LAT), F32),
            pltpu.VMEM((2, toks, KVW), BF16),
            pltpu.VMEM((2 * q_rows, Q_LAT), BF16),
            pltpu.VMEM((2, q_rows, toks), F32),
            pltpu.VMEM((2, 2, toks, LANES), BF16),
            pltpu.VMEM((n_qu, 2 * q_rows, QU_HEADS * QK_DIM), BF16),
            pltpu.VMEM((2, toks, KU_HEADS * KV_DIM), BF16),
            pltpu.VMEM((2, toks, KU_HEADS * KV_DIM), BF16),
            pltpu.VMEM((units, q_rows, toks), F32),
            pltpu.VMEM((units, q_rows, toks), F32),
            pltpu.VMEM((units, q_rows, toks), BF16),
            pltpu.VMEM((units, q_rows, toks), BF16),
            pltpu.VMEM((2 * q_rows, heads * V_DIM), BF16),
            pltpu.VMEM((2 * q_rows, COLS), F32),
            pltpu.VMEM((2, 2 * q_rows, COLS), BF16),
            dma((2,)), dma((2,)), dma((2,)), dma((2,)), dma((1,)), dma((1,)),
            dma((RING,)), dma((n_down, 2)), dma((QU_SLOTS,)), dma((KU_SLOTS,)),
            dma((14,)), dma((7, 2)),
            dma((1,)), dma((1,)),
            dma((n_ku // 2,)), dma((n_ku // 2,)),
            dma((2, 2)), dma((2, 2)), dma((n_wo_n, 2)),
        ],
        compiler_params=pltpu.CompilerParams(
            collective_id=0, has_side_effects=True, vmem_limit_bytes=67043328),
        name="mla",
    )(x_one, x_two, pos_one, pos_two, freq, w_qd, gain_q, w_qu, w_kvd, gain_kv, w_kvu, w_out)


def solution(mesh):
    tok_spec = P(('dp', 'sp'), None)
    idx_spec = P(('dp', 'sp'))
    n_sp = mesh.shape['sp']
    freq = ROPE_BASE ** (-(np.arange(LANES) % HALF_ROPE).astype(np.float64) / HALF_ROPE)
    freq = freq.astype(np.float32)[None, :]

    def local_body(x_one, seg_one, pos_one, x_two, seg_two, pos_two, w_qdown, gain_q, w_qup, w_kvdown, gain_kv, w_kvup, w_out):
        return mla(n_sp, x_one, x_two, pos_one, pos_two, jnp.asarray(freq), w_qdown, gain_q, w_qup, w_kvdown.T, gain_kv, w_kvup, w_out)

    return jax.shard_map(local_body, mesh=mesh, in_specs=(tok_spec, idx_spec, idx_spec, tok_spec, idx_spec, idx_spec) + (P(),) * 7, out_specs=(tok_spec, tok_spec), check_vma=False)
```

```python
import functools

import jax
import jax.numpy as jnp
import numpy as np
from jax import lax
from jax.experimental import pallas as pl
from jax.experimental.pallas import tpu as pltpu
from jax.sharding import PartitionSpec as P

NOPE_DIM = 128
ROPE_DIM = 64
HALF_ROPE = 32
KV_LAT = 512
Q_LAT = 1536
V_DIM = 128
QK_DIM = NOPE_DIM + ROPE_DIM
KV_DIM = NOPE_DIM + V_DIM
ROPE_BASE = 10000.0
NORM_EPS = 1e-6
LANES = 128

ROWS = 1024
COLS = 512
RING = 25
WO_RING = 24
QU_HEADS = 4
QU_SLOTS = 2
RING_QU = 6
AHEAD = 4
KU_HEADS = 2
KU_SLOTS = 4
KVW = KV_LAT + LANES
MASKED = -1e30
BIG = 3e38
F32 = jnp.float32
BF16 = jnp.bfloat16


def body(n_sp, heads, d_model, blk,
         x_one, x_two, pos_one, pos_two, freq, w_qd, gain_q, w_qu, w_kvd, gain_kv, w_kvu, w_out,
         y_one, y_two,
         x_all, pos_s, ends, pos_all, trig, ring, qu, ku, acc_kv, acc_q, kv_all, cq_all,
         cap, kr, q_s, f_s, kvs0, kvs1, s0, s1, p0, p1, o_all, y_st,
         x_sem, x_ss, x_rs, pos_sem, pos_ss, pos_rs, kvd_sem, qd_sem, qu_sem, ku_sem, wo_sem,
         kv_ss, kv_rs, cq_ss, cq_rs, o_ss, o_rs, y_ls, y_ss, y_rs):
    me = lax.axis_index("sp")
    core = lax.rem(me, 2)
    chip = me // 2
    pair = me + 1 - 2 * core
    right = lax.rem(me + 2, n_sp)
    left = lax.rem(me + n_sp - 2, n_sp)
    opp = lax.rem(me + 4, n_sp)
    q_rows = 2 * blk
    toks = n_sp * blk
    half_heads = heads // 2
    y_cols = d_model // 2
    n_down = d_model // ROWS
    q_cols = Q_LAT // 2
    n_kvd = d_model // COLS
    n_qu = half_heads // QU_HEADS
    n_ku = half_heads // KU_HEADS
    n_wo_k = heads * V_DIM // ROWS // 2
    n_wo_n = y_cols // COLS
    n_wo = 2 * n_wo_n
    n_part = WO_RING // n_wo_k

    def rcopy(src, dst, ss, rs, dev):
        return pltpu.make_async_remote_copy(
            src_ref=src, dst_ref=dst, send_sem=ss, recv_sem=rs,
            device_id={"sp": dev}, device_id_type=pl.DeviceIdType.MESH)

    def ds(start, size):
        return pl.ds(start if isinstance(start, int) else pl.multiple_of(start, size), size)

    half = COLS // 2

    def kvd_copy(k):
        dst = ring.at[k, pl.ds(0, KV_LAT + ROPE_DIM)]
        return pltpu.make_async_copy(w_kvd.at[:, ds(k * COLS, COLS)], dst, kvd_sem.at[k])

    def qd_refs(k):
        return ring.at[n_kvd + k], ring.at[n_kvd + n_down + k // 2, :, ds(lax.rem(k, 2) * half, half)]

    def qd_copies(k):
        col = core * q_cols
        rows = ds(k * ROWS, ROWS)
        one, two = qd_refs(k)
        return (pltpu.make_async_copy(w_qd.at[rows, pl.ds(pl.multiple_of(col, half), COLS)], one, qd_sem.at[k, 0]),
                pltpu.make_async_copy(w_qd.at[rows, pl.ds(pl.multiple_of(col + COLS, half), half)], two, qd_sem.at[k, 1]))

    low_rows = Q_LAT - ROWS

    def qu_parts(i):
        width = QU_HEADS * QK_DIM
        if i >= RING_QU:
            return [((0, 0, Q_LAT, width), qu.at[(i - RING_QU) % QU_SLOTS])]
        rest = width - COLS
        return [((0, 0, ROWS, COLS), ring.at[3 * i]),
                ((0, COLS, ROWS, rest), ring.at[3 * i + 1, :, pl.ds(0, rest)]),
                ((ROWS, 0, low_rows, COLS), ring.at[3 * i + 2, pl.ds(0, low_rows)]),
                ((ROWS, COLS, low_rows, rest), ring.at[3 * i + 2, pl.ds(low_rows, low_rows), pl.ds(0, rest)])]

    def qu_copies(i):
        base = core * (half_heads * QK_DIM) + i * (QU_HEADS * QK_DIM)
        out = []
        for n, ((r, c, nr, nc), dst) in enumerate(qu_parts(i)):
            cols = pl.ds(pl.multiple_of(base + c, half), nc)
            out.append(pltpu.make_async_copy(w_qu.at[pl.ds(r, nr), cols], dst, qu_sem.at[i, n]))
        return out

    def qu_dot(i):
        parts = [dst[...] for _, dst in qu_parts(i)]
        if len(parts) == 1:
            return jnp.dot(cq_all[...], parts[0], preferred_element_type=F32)
        top = jnp.concatenate(parts[:2], axis=1)
        bottom = jnp.concatenate(parts[2:], axis=1)
        return (jnp.dot(cq_all[:, :ROWS], top, preferred_element_type=F32)
                + jnp.dot(cq_all[:, ROWS:], bottom, preferred_element_type=F32))

    def ku_copy(i):
        width = KU_HEADS * KV_DIM
        cols = ds(core * (half_heads * KV_DIM) + i * width, width)
        slot = lax.rem(i, KU_SLOTS)
        return pltpu.make_async_copy(w_kvu.at[:, cols], ku.at[slot], ku_sem.at[slot])

    def wo_part(g):
        return pl.ds(g % n_part * n_wo_k if isinstance(g, int) else lax.rem(g, n_part) * n_wo_k, n_wo_k)

    def wo_copy(g):
        side = lax.rem(core + g, 2)
        cols = ds(core * y_cols + g // 2 * COLS, COLS)
        return pltpu.make_async_copy(w_out.at[ds(side * n_wo_k, n_wo_k), :, cols], ring.at[wo_part(g)], wo_sem.at[lax.rem(g, n_part)])

    x_in = (x_one, x_two)

    def x_rows(m, c):
        return ds(c * q_rows + m * blk, blk)

    def my_rows(m, c):
        return ds(m * q_rows + c * blk, blk)

    pos_cp = [pltpu.make_async_copy((pos_one, pos_two)[m], pos_s.at[m], pos_sem.at[m]) for m in range(2)]
    x_cp = [pltpu.make_async_copy(x_in[m], x_all.at[x_rows(m, core)], x_sem.at[m]) for m in range(2)]
    for c in pos_cp + x_cp:
        c.start()
    stream = [[kvd_copy(2 * k), kvd_copy(2 * k + 1)] for k in range(n_down)]
    stream += [qd_copies(k) for k in range(n_down)]
    stream += [qu_copies(i) for i in range(RING_QU + QU_SLOTS)]
    issued = []

    def issue(count):
        for _ in range(count):
            if len(issued) < len(stream):
                for c in stream[len(issued)]:
                    c.start()
                issued.append(None)

    issue(AHEAD)

    barrier = pltpu.get_barrier_semaphore()
    for dev in (pair, left, right):
        pl.semaphore_signal(barrier, inc=1, device_id={"sp": dev}, device_id_type=pl.DeviceIdType.MESH)
    for c in pos_cp:
        c.wait()
    for m in range(2):
        first, final = pos_s[m, 0], pos_s[m, blk - 1]
        ends[core, 2 * m] = jnp.full((8, LANES), first, jnp.int32).astype(F32)
        ends[core, 2 * m + 1] = jnp.full((8, LANES), final, jnp.int32).astype(F32)

    lane = lax.broadcasted_iota(jnp.int32, (blk, LANES), 1)
    first_half = lax.rem(lane, ROPE_DIM) < HALF_ROPE

    def positions(m, c):
        tok = lax.broadcasted_iota(jnp.int32, (blk, LANES), 0).astype(F32)
        first = jnp.concatenate([ends[c, 2 * m]] * (blk // 8), axis=0)
        back = jnp.concatenate([ends[c, 2 * m + 1]] * (blk // 8), axis=0) - (blk - 1)
        val = jnp.where(tok + back >= 0, tok + back, tok + first)
        rows = my_rows(m, c)
        pos_all[rows, :] = val
        ang = val * freq[...]
        sin = jnp.sin(ang)
        trig[0, rows, :] = jnp.cos(ang)
        trig[1, rows, :] = jnp.where(first_half, -sin, sin)

    for m in range(2):
        positions(m, core)
    pl.semaphore_wait(barrier, 3)
    x_rc = [rcopy(x_in[m], x_all.at[x_rows(m, core)], x_ss.at[m], x_rs.at[m], pair) for m in range(2)]
    for c in x_rc:
        c.start()
    ends_rc = rcopy(ends.at[core], ends.at[core], pos_ss.at[0], pos_rs.at[0], pair)
    for c in x_cp:
        c.wait()

    my_x = ds(core * q_rows, q_rows)
    lat_rows = KV_LAT + ROPE_DIM
    u = [None, None]
    for k in range(n_down):
        for c in range(2):
            kvd_copy(2 * k + c).wait()
        issue(3 if k == n_down - 1 else 1)
        x_k = x_all[my_x, ds(k * ROWS, ROWS)]
        for h, (a, b) in enumerate(((0, lat_rows // 2), (lat_rows // 2, lat_rows))):
            w_k = jnp.concatenate([ring[2 * k, a:b], ring[2 * k + 1, a:b]], axis=1)
            d = lax.dot_general(w_k, x_k, (((1,), (1,)), ((), ())), preferred_element_type=F32)
            u[h] = d if k == 0 else u[h] + d
    acc_kv[:lat_rows // 2, :] = u[0]
    acc_kv[lat_rows // 2:lat_rows, :] = u[1]
    acc_kv[lat_rows:, :] = u[1][lat_rows // 2 - ROPE_DIM:, :]
    lat_all = acc_kv[...].T
    ends_rc.start()

    def rotate(z, cos, sin, sel):
        swapped = jnp.where(sel, pltpu.roll(z, LANES - HALF_ROPE, 1), pltpu.roll(z, HALF_ROPE, 1))
        return z * cos + swapped * sin

    own = ds(me * blk, blk)
    for m in range(2):
        lat = lat_all[m * blk:(m + 1) * blk, :KV_LAT]
        inv = lax.rsqrt(jnp.mean(lat * lat, axis=-1, keepdims=True) + NORM_EPS)
        kv_all[m, own, :KV_LAT] = (lat * inv * gain_kv[...].astype(F32).reshape(1, -1)).astype(BF16)
        raw = lat_all[m * blk:(m + 1) * blk, KV_LAT:]
        kv_all[m, own, KV_LAT:] = rotate(raw, trig[0, my_rows(m, core), :], trig[1, my_rows(m, core), :], first_half).astype(BF16)

    def piece(m, dev):
        return kv_all.at[m, ds(dev * blk, blk)]

    def kv_send(i, m, src_dev, role, dev):
        return rcopy(piece(m, src_dev), piece(m, src_dev), kv_ss.at[i], kv_rs.at[role, m], dev)

    def kv_wait(m, src_dev, role):
        rcopy(piece(m, src_dev), piece(m, src_dev), kv_ss.at[0], kv_rs.at[role, m], pair).wait_recv()

    sends = []
    for m in range(2):
        sends.append(kv_send(len(sends), m, me, 2, left))
        sends.append(kv_send(len(sends), m, me, 1, right))
    for m in range(2):
        sends.append(kv_send(len(sends), m, me, 0, pair))
    for c in sends:
        c.start()
    for c in x_rc:
        c.wait_recv()
    my_cols = ds(core * q_cols, q_cols)
    z = [None, None]
    for k in range(n_down):
        for c in qd_copies(k):
            c.wait()
        issue(4 if k == n_down - 1 else 1)
        one, two = qd_refs(k)
        w_k = jnp.concatenate([one[...], two[...]], axis=1)
        for h in range(2):
            d = jnp.dot(x_all[h * q_rows:(h + 1) * q_rows, k * ROWS:(k + 1) * ROWS], w_k, preferred_element_type=F32)
            z[h] = d if k == 0 else z[h] + d
    for h in range(2):
        acc_q[h * q_rows:(h + 1) * q_rows, my_cols] = z[h]
    for i in range(KU_SLOTS):
        ku_copy(i).start(priority=1)
    cq_rc = rcopy(acc_q.at[:, my_cols], acc_q.at[:, my_cols], cq_ss.at[0], cq_rs.at[0], pair)
    cq_rc.start()

    ends_rc.wait_recv()
    for m in range(2):
        positions(m, 1 - core)
    for m in range(2):
        row = lax.broadcasted_iota(jnp.int32, (q_rows, LANES), 0) + chip * q_rows
        start = row.astype(F32) - pos_all[m * q_rows:(m + 1) * q_rows, :]
        for c in range(toks // LANES):
            key = lax.broadcasted_iota(jnp.int32, (q_rows, LANES), 1) + c * LANES
            keep = (key <= row) & (key.astype(F32) >= start)
            cap[m, :, c * LANES:(c + 1) * LANES] = jnp.where(keep, BIG, MASKED)

    cq_rc.wait_recv()
    cq_rc.wait_send()
    for m in range(2):
        for c in range(2):
            lat = acc_q[c * q_rows + m * blk:c * q_rows + (m + 1) * blk, :]
            inv = lax.rsqrt(jnp.mean(lat * lat, axis=-1, keepdims=True) + NORM_EPS)
            cq_all[my_rows(m, c), :] = (lat * inv * gain_q[...].astype(F32).reshape(1, -1)).astype(BF16)

    second = []
    for m in range(2):
        kv_wait(m, left, 1)
        kv_wait(m, right, 2)
    second.append(kv_send(6, 0, left, 3, right))
    second.append(kv_send(7, 1, right, 3, left))
    for m in range(2):
        second.append(kv_send(8 + m, m, left, 4, pair))
        second.append(kv_send(10 + m, m, right, 5, pair))
    for c in second:
        c.start()
    sends += second

    lane2 = lax.broadcasted_iota(jnp.int32, (2 * q_rows, LANES), 1)
    first_half2 = lax.rem(lane2, ROPE_DIM) < HALF_ROPE
    low = lane2 < ROPE_DIM

    f_buf = (acc_q, f_s)
    f_width = QU_HEADS * QK_DIM

    def q_post(t):
        for p in range(QU_HEADS):
            i, base = 2 * t + p // 2, 2 * QK_DIM * (p % 2)
            t0, t1, t2 = (f_buf[t % 2][:, 2 * QK_DIM * p + LANES * n:2 * QK_DIM * p + LANES * (n + 1)] for n in range(3))
            q_s[i, :, base:base + LANES] = t0.astype(BF16)
            q_s[i, :, base + LANES:base + 2 * LANES] = pltpu.roll(jnp.where(low, t2, t1), ROPE_DIM, 1).astype(BF16)
            q_s[i, :, base + 2 * LANES:base + 3 * LANES] = rotate(jnp.where(low, t1, t2), trig[0], trig[1], first_half2).astype(BF16)

    for t in range(n_qu // 2):
        for i in (2 * t, 2 * t + 1):
            for c in qu_copies(i):
                c.wait()
        for i in (2 * t - 2, 2 * t - 1):
            if i >= RING_QU and i + QU_SLOTS < n_qu:
                for c in qu_copies(i + QU_SLOTS):
                    c.start()
        if t == n_qu // 2 - 1:
            third = []
            for m in range(2):
                kv_wait(m, opp, 3)
                third.append(kv_send(12 + m, m, opp, 6, pair))
            for c in third:
                c.start()
            sends += third
        for h in range(2):
            f_buf[t % 2][:, h * f_width:(h + 1) * f_width] = qu_dot(2 * t + h)
        if t > 0:
            q_post(t - 1)
    wo_copy(0).start(priority=1)
    q_post(n_qu // 2 - 1)

    other = 1 - 2 * core
    for m in range(2):
        kv_wait(m, pair, 0)
        kv_wait(m, left + other, 4)
        kv_wait(m, right + other, 5)
        kv_wait(m, opp + other, 6)
    lane3 = lax.broadcasted_iota(jnp.int32, (toks, LANES), 1)
    for m in range(2):
        t = kv_all[m, :, KV_LAT:].astype(F32)
        kr[0, m] = jnp.where(lane3 < ROPE_DIM, t, 0.0).astype(BF16)
        kr[1, m] = jnp.where(lane3 < ROPE_DIM, 0.0, t).astype(BF16)

    exp_scale = QK_DIM ** -0.5 * 1.4426950408889634
    kvs, s_scr, p_scr = (kvs0, kvs1), (s0, s1), (p0, p1)
    o_width = 2 * KU_HEADS * V_DIM

    def o_copy(t):
        cols = ds(t * o_width, o_width)
        return rcopy(o_all.at[core, :, cols], o_all.at[core, :, cols], o_ss.at[t], o_rs.at[t], pair)

    def kv_up(b, i):
        for m in range(2):
            kvs[b][m] = jnp.dot(kv_all[m, :, :KV_LAT], ku[lax.rem(i, KU_SLOTS)], preferred_element_type=F32).astype(BF16)

    def scores(b, t):
        for m in range(2):
            rows = slice(m * q_rows, (m + 1) * q_rows)
            for j in range(KU_HEADS):
                base = 2 * QK_DIM * b
                nope = q_s[t, rows, base + LANES * j:base + LANES * (j + 1)]
                rope = q_s[t, rows, base + 2 * LANES:base + 3 * LANES]
                qc = jnp.concatenate([nope, rope], axis=1)
                kc = jnp.concatenate([kvs[b][m, :, KV_DIM * j:KV_DIM * j + NOPE_DIM], kr[j, m]], axis=1)
                s_scr[b][KU_HEADS * m + j] = lax.dot_general(qc, kc, (((1,), (1,)), ((), ())), preferred_element_type=F32)

    def softmax(b):
        step = 32
        for m in range(2):
            for j in range(KU_HEADS):
                for r in range(q_rows // step):
                    rows = slice(r * step, (r + 1) * step)
                    s = jnp.minimum(s_scr[b][KU_HEADS * m + j, rows, :], cap[m, rows, :])
                    top = jnp.max(s, axis=-1, keepdims=True)
                    e = jnp.exp2((s - top) * exp_scale)
                    inv = 1.0 / jnp.sum(e, axis=-1, keepdims=True)
                    p_scr[b][KU_HEADS * m + j, rows, :] = (e * inv).astype(BF16)

    def values(b, t):
        for m in range(2):
            rows = slice(m * q_rows, (m + 1) * q_rows)
            for j in range(KU_HEADS):
                v = kvs[b][m, :, KV_DIM * j + NOPE_DIM:KV_DIM * (j + 1)]
                o = jnp.dot(p_scr[b][KU_HEADS * m + j], v, preferred_element_type=F32).astype(BF16)
                col = t * o_width + (KU_HEADS * b + j) * V_DIM
                o_all[core, rows, ds(col, V_DIM)] = o

    ku_copy(0).wait()
    kv_up(0, 0)
    scores(0, 0)
    ku_copy(KU_SLOTS).start()
    n_loop = n_ku // 2 - 1

    def at_step(t, carry):
        ku_copy(2 * t + 1).wait()
        ku_copy(2 * t + 2).wait()
        softmax(0)
        kv_up(1, 2 * t + 1)
        values(0, t)
        scores(1, t)
        softmax(1)
        kv_up(0, 2 * t + 2)
        values(1, t)
        scores(0, t + 1)
        for d in (5, 6):
            @pl.when(2 * t + d < n_ku)
            def _():
                ku_copy(2 * t + d).start()
        @pl.when(t + 1 < n_part)
        def _():
            wo_copy(t + 1).start(priority=1)

        o_copy(t).start()
        return carry

    lax.fori_loop(0, n_loop, at_step, 0)
    last = n_loop
    ku_copy(n_ku - 1).wait()
    softmax(0)
    kv_up(1, n_ku - 1)
    values(0, last)
    scores(1, last)
    softmax(1)
    values(1, last)
    o_copy(last).start()

    y_out = (y_one, y_two)

    def y_copies(n):
        slot = n % 2
        cols = ds(core * y_cols + n * COLS, COLS)
        local = [pltpu.make_async_copy(y_st.at[slot, my_rows(m, core)], y_out[m].at[:, cols], y_ls.at[slot, m]) for m in range(2)]
        remote = [rcopy(y_st.at[slot, my_rows(m, 1 - core)], y_out[m].at[:, cols], y_ss.at[slot, m], y_rs.at[n, m], pair) for m in range(2)]
        return local, remote

    def y_wait(n):
        local, remote = y_copies(n)
        for m in range(2):
            local[m].wait()
            remote[m].wait_send()

    def half_dot(g):
        side = lax.rem(core + g, 2)
        w_g = ring[wo_part(g)].reshape(n_wo_k * ROWS, COLS)
        return jnp.dot(o_all[side], w_g, preferred_element_type=F32)

    def y_start(n):
        local, remote = y_copies(n)
        for m in range(2):
            remote[m].start()
            local[m].start()

    wo_copy(0).wait()
    acc = half_dot(0)
    for t in range(n_loop + 1):
        cols = ds(t * o_width, o_width)
        rcopy(o_all.at[1 - core, :, cols], o_all.at[1 - core, :, cols], o_ss.at[t], o_rs.at[t], pair).wait_recv()
    wo_copy(1).wait()
    acc = acc + half_dot(1)
    for n in range(1, n_wo_n + 1):
        if n < n_wo_n:
            for g in (2 * n, 2 * n + 1):
                wo_copy(g).wait()
        if n >= 2:
            y_start(n - 2)
        if n >= 3:
            y_wait(n - 3)
        for g in (2 * n - 2 + n_part, 2 * n - 1 + n_part):
            if g < n_wo:
                wo_copy(g).start()
        y_st[(n - 1) % 2] = acc.astype(BF16)
        if n < n_wo_n:
            acc = half_dot(2 * n) + half_dot(2 * n + 1)
    y_start(n_wo_n - 1)
    y_wait(n_wo_n - 2)
    y_wait(n_wo_n - 1)
    for n in range(n_wo_n):
        cols = ds((1 - core) * y_cols + n * COLS, COLS)
        for m in range(2):
            rcopy(y_st.at[0, my_rows(m, core)], y_out[m].at[:, cols], y_ss.at[0, m], y_rs.at[n, m], pair).wait_recv()
    for c in x_rc + [ends_rc]:
        c.wait_send()
    for c in sends:
        c.wait_send()
    for t in range(n_loop + 1):
        o_copy(t).wait_send()


def mla(n_sp, x_one, x_two, pos_one, pos_two, freq, w_qd, gain_q, w_qu, w_kvd, gain_kv, w_kvu, w_out):
    blk, d_model = x_one.shape
    heads = w_out.shape[0] * w_out.shape[1] // V_DIM
    toks = n_sp * blk
    q_rows = 2 * blk
    n_down = d_model // ROWS
    n_qu = heads // 2 // QU_HEADS
    n_ku = heads // 2 // KU_HEADS
    n_wo_n = d_model // 2 // COLS
    hbm = pl.BlockSpec(memory_space=pl.ANY)
    vmem = pl.BlockSpec(memory_space=pltpu.VMEM)
    dma = pltpu.SemaphoreType.DMA
    units = 2 * KU_HEADS
    return pl.pallas_call(
        functools.partial(body, n_sp, heads, d_model, blk),
        out_shape=[jax.ShapeDtypeStruct((blk, d_model), BF16)] * 2,
        in_specs=[hbm, hbm, hbm, hbm, vmem, hbm, vmem, hbm, hbm, vmem, hbm, hbm],
        out_specs=[hbm, hbm],
        scratch_shapes=[
            pltpu.VMEM((2 * q_rows, d_model), BF16),
            pltpu.SMEM((2, blk), jnp.int32),
            pltpu.VMEM((2, 4, 8, LANES), F32),
            pltpu.VMEM((2 * q_rows, LANES), F32),
            pltpu.VMEM((2, 2 * q_rows, LANES), F32),
            pltpu.VMEM((RING, ROWS, COLS), BF16),
            pltpu.VMEM((QU_SLOTS, Q_LAT, QU_HEADS * QK_DIM), BF16),
            pltpu.VMEM((KU_SLOTS, KV_LAT, KU_HEADS * KV_DIM), BF16),
            pltpu.VMEM((KV_LAT + 2 * ROPE_DIM, 2 * blk), F32),
            pltpu.VMEM((2 * q_rows, Q_LAT), F32),
            pltpu.VMEM((2, toks, KVW), BF16),
            pltpu.VMEM((2 * q_rows, Q_LAT), BF16),
            pltpu.VMEM((2, q_rows, toks), F32),
            pltpu.VMEM((2, 2, toks, LANES), BF16),
            pltpu.VMEM((n_qu, 2 * q_rows, QU_HEADS * QK_DIM), BF16),
            pltpu.VMEM((2 * q_rows, 2 * QU_HEADS * QK_DIM), F32),
            pltpu.VMEM((2, toks, KU_HEADS * KV_DIM), BF16),
            pltpu.VMEM((2, toks, KU_HEADS * KV_DIM), BF16),
            pltpu.VMEM((units, q_rows, toks), F32),
            pltpu.VMEM((units, q_rows, toks), F32),
            pltpu.VMEM((units, q_rows, toks), BF16),
            pltpu.VMEM((units, q_rows, toks), BF16),
            pltpu.VMEM((2, 2 * q_rows, heads // 2 * V_DIM), BF16),
            pltpu.VMEM((2, 2 * q_rows, COLS), BF16),
            dma((2,)), dma((2,)), dma((2,)), dma((2,)), dma((1,)), dma((1,)),
            dma((d_model // COLS,)), dma((n_down, 2)), dma((n_qu, 4)), dma((KU_SLOTS,)), dma((WO_RING,)),
            dma((14,)), dma((7, 2)),
            dma((1,)), dma((1,)),
            dma((n_ku // 2,)), dma((n_ku // 2,)),
            dma((2, 2)), dma((2, 2)), dma((n_wo_n, 2)),
        ],
        compiler_params=pltpu.CompilerParams(
            collective_id=0, has_side_effects=True, vmem_limit_bytes=67043328),
        name="mla",
    )(x_one, x_two, pos_one, pos_two, freq, w_qd, gain_q, w_qu, w_kvd, gain_kv, w_kvu, w_out)


def solution(mesh):
    tok_spec = P(('dp', 'sp'), None)
    idx_spec = P(('dp', 'sp'))
    n_sp = mesh.shape['sp']
    freq = ROPE_BASE ** (-(np.arange(LANES) % HALF_ROPE).astype(np.float64) / HALF_ROPE)
    freq = freq.astype(np.float32)[None, :]

    def local_body(x_one, seg_one, pos_one, x_two, seg_two, pos_two, w_qdown, gain_q, w_qup, w_kvdown, gain_kv, w_kvup, w_out):
        return mla(n_sp, x_one, x_two, pos_one, pos_two, jnp.asarray(freq), w_qdown, gain_q, w_qup, w_kvdown.T, gain_kv, w_kvup, w_out.reshape(-1, ROWS, w_out.shape[1]))

    return jax.shard_map(local_body, mesh=mesh, in_specs=(tok_spec, idx_spec, idx_spec, tok_spec, idx_spec, idx_spec) + (P(),) * 7, out_specs=(tok_spec, tok_spec), check_vma=False)
```

```python
import functools

import jax
import jax.numpy as jnp
import numpy as np
from jax import lax
from jax.experimental import pallas as pl
from jax.experimental.pallas import tpu as pltpu
from jax.sharding import PartitionSpec as P

NOPE_DIM = 128
ROPE_DIM = 64
HALF_ROPE = 32
KV_LAT = 512
Q_LAT = 1536
V_DIM = 128
QK_DIM = NOPE_DIM + ROPE_DIM
KV_DIM = NOPE_DIM + V_DIM
ROPE_BASE = 10000.0
NORM_EPS = 1e-6
LANES = 128

ROWS = 1024
COLS = 512
RING = 25
WO_RING = 24
QU_HEADS = 4
QU_SLOTS = 2
RING_QU = 6
AHEAD = 4
KU_HEADS = 2
KU_SLOTS = 4
KVW = KV_LAT + LANES
MASKED = -1e30
BIG = 3e38
F32 = jnp.float32
BF16 = jnp.bfloat16


def body(n_sp, heads, d_model, blk,
         x_one, x_two, pos_one, pos_two, freq, w_qd, gain_q, w_qu, w_kvd, gain_kv, w_kvu, w_out,
         y_one, y_two,
         x_all, pos_s, ends, pos_all, trig, ring, qu, ku, acc_kv, acc_q, kv_all, cq_all,
         cap, kr, q_s, f_s, kvs0, kvs1, s0, s1, p0, p1, o_all, y_st,
         x_sem, x_ss, x_rs, pos_sem, pos_ss, pos_rs, kvd_sem, qd_sem, qu_sem, ku_sem, wo_sem,
         kv_ss, kv_rs, cq_ss, cq_rs, o_ss, o_rs, y_ls, y_ss, y_rs):
    me = lax.axis_index("sp")
    core = lax.rem(me, 2)
    chip = me // 2
    pair = me + 1 - 2 * core
    right = lax.rem(me + 2, n_sp)
    left = lax.rem(me + n_sp - 2, n_sp)
    opp = lax.rem(me + 4, n_sp)
    q_rows = 2 * blk
    toks = n_sp * blk
    half_heads = heads // 2
    y_cols = d_model // 2
    n_down = d_model // ROWS
    q_cols = Q_LAT // 2
    n_kvd = d_model // COLS
    n_qu = half_heads // QU_HEADS
    n_ku = half_heads // KU_HEADS
    n_wo_k = heads * V_DIM // ROWS // 2
    n_wo_n = y_cols // COLS
    n_wo = 2 * n_wo_n
    n_part = WO_RING // n_wo_k

    def rcopy(src, dst, ss, rs, dev):
        return pltpu.make_async_remote_copy(
            src_ref=src, dst_ref=dst, send_sem=ss, recv_sem=rs,
            device_id={"sp": dev}, device_id_type=pl.DeviceIdType.MESH)

    def ds(start, size):
        return pl.ds(start if isinstance(start, int) else pl.multiple_of(start, size), size)

    half = COLS // 2

    def kvd_copy(k):
        dst = ring.at[k, pl.ds(0, KV_LAT + ROPE_DIM)]
        return pltpu.make_async_copy(w_kvd.at[:, ds(k * COLS, COLS)], dst, kvd_sem.at[k])

    def qd_refs(k):
        return ring.at[n_kvd + k], ring.at[n_kvd + n_down + k // 2, :, ds(lax.rem(k, 2) * half, half)]

    def qd_copies(k):
        col = core * q_cols
        rows = ds(k * ROWS, ROWS)
        one, two = qd_refs(k)
        return (pltpu.make_async_copy(w_qd.at[rows, pl.ds(pl.multiple_of(col, half), COLS)], one, qd_sem.at[k, 0]),
                pltpu.make_async_copy(w_qd.at[rows, pl.ds(pl.multiple_of(col + COLS, half), half)], two, qd_sem.at[k, 1]))

    low_rows = Q_LAT - ROWS

    def qu_parts(i):
        width = QU_HEADS * QK_DIM
        if i >= RING_QU:
            return [((0, 0, Q_LAT, width), qu.at[(i - RING_QU) % QU_SLOTS])]
        rest = width - COLS
        return [((0, 0, ROWS, COLS), ring.at[3 * i]),
                ((0, COLS, ROWS, rest), ring.at[3 * i + 1, :, pl.ds(0, rest)]),
                ((ROWS, 0, low_rows, COLS), ring.at[3 * i + 2, pl.ds(0, low_rows)]),
                ((ROWS, COLS, low_rows, rest), ring.at[3 * i + 2, pl.ds(low_rows, low_rows), pl.ds(0, rest)])]

    def qu_copies(i):
        base = core * (half_heads * QK_DIM) + i * (QU_HEADS * QK_DIM)
        out = []
        for n, ((r, c, nr, nc), dst) in enumerate(qu_parts(i)):
            cols = pl.ds(pl.multiple_of(base + c, half), nc)
            out.append(pltpu.make_async_copy(w_qu.at[pl.ds(r, nr), cols], dst, qu_sem.at[i, n]))
        return out

    def qu_dot(i):
        parts = [dst[...] for _, dst in qu_parts(i)]
        if len(parts) == 1:
            return jnp.dot(cq_all[...], parts[0], preferred_element_type=F32)
        top = jnp.concatenate(parts[:2], axis=1)
        bottom = jnp.concatenate(parts[2:], axis=1)
        return (jnp.dot(cq_all[:, :ROWS], top, preferred_element_type=F32)
                + jnp.dot(cq_all[:, ROWS:], bottom, preferred_element_type=F32))

    def ku_copy(i):
        width = KU_HEADS * KV_DIM
        cols = ds(core * (half_heads * KV_DIM) + i * width, width)
        slot = lax.rem(i, KU_SLOTS)
        return pltpu.make_async_copy(w_kvu.at[:, cols], ku.at[slot], ku_sem.at[slot])

    def wo_part(g):
        return pl.ds(g % n_part * n_wo_k if isinstance(g, int) else lax.rem(g, n_part) * n_wo_k, n_wo_k)

    def wo_copy(g):
        side = lax.rem(core + g, 2)
        cols = ds(core * y_cols + g // 2 * COLS, COLS)
        return pltpu.make_async_copy(w_out.at[ds(side * n_wo_k, n_wo_k), :, cols], ring.at[wo_part(g)], wo_sem.at[lax.rem(g, n_part)])

    x_in = (x_one, x_two)

    def x_rows(m, c):
        return ds(c * q_rows + m * blk, blk)

    def my_rows(m, c):
        return ds(m * q_rows + c * blk, blk)

    pos_cp = [pltpu.make_async_copy((pos_one, pos_two)[m], pos_s.at[m], pos_sem.at[m]) for m in range(2)]
    x_cp = [pltpu.make_async_copy(x_in[m], x_all.at[x_rows(m, core)], x_sem.at[m]) for m in range(2)]
    for c in pos_cp + x_cp:
        c.start()
    stream = [[kvd_copy(2 * k), kvd_copy(2 * k + 1)] for k in range(n_down)]
    stream += [qd_copies(k) for k in range(n_down)]
    stream += [qu_copies(i) for i in range(RING_QU + QU_SLOTS)]
    issued = []

    def issue(count):
        for _ in range(count):
            if len(issued) < len(stream):
                for c in stream[len(issued)]:
                    c.start()
                issued.append(None)

    issue(AHEAD)

    barrier = pltpu.get_barrier_semaphore()
    for dev in (pair, left, right):
        pl.semaphore_signal(barrier, inc=1, device_id={"sp": dev}, device_id_type=pl.DeviceIdType.MESH)
    for c in pos_cp:
        c.wait()
    for m in range(2):
        first, final = pos_s[m, 0], pos_s[m, blk - 1]
        ends[core, 2 * m] = jnp.full((8, LANES), first, jnp.int32).astype(F32)
        ends[core, 2 * m + 1] = jnp.full((8, LANES), final, jnp.int32).astype(F32)

    lane = lax.broadcasted_iota(jnp.int32, (blk, LANES), 1)
    first_half = lax.rem(lane, ROPE_DIM) < HALF_ROPE

    def positions(m, c):
        tok = lax.broadcasted_iota(jnp.int32, (blk, LANES), 0).astype(F32)
        first = jnp.concatenate([ends[c, 2 * m]] * (blk // 8), axis=0)
        back = jnp.concatenate([ends[c, 2 * m + 1]] * (blk // 8), axis=0) - (blk - 1)
        val = jnp.where(tok + back >= 0, tok + back, tok + first)
        rows = my_rows(m, c)
        pos_all[rows, :] = val
        ang = val * freq[...]
        sin = jnp.sin(ang)
        trig[0, rows, :] = jnp.cos(ang)
        trig[1, rows, :] = jnp.where(first_half, -sin, sin)

    for m in range(2):
        positions(m, core)
    pl.semaphore_wait(barrier, 3)
    x_rc = [rcopy(x_in[m], x_all.at[x_rows(m, core)], x_ss.at[m], x_rs.at[m], pair) for m in range(2)]
    for c in x_rc:
        c.start()
    ends_rc = rcopy(ends.at[core], ends.at[core], pos_ss.at[0], pos_rs.at[0], pair)
    for c in x_cp:
        c.wait()

    my_x = ds(core * q_rows, q_rows)
    lat_rows = KV_LAT + ROPE_DIM
    u = [None, None]
    for k in range(n_down):
        for c in range(2):
            kvd_copy(2 * k + c).wait()
        issue(3 if k == n_down - 1 else 1)
        x_k = x_all[my_x, ds(k * ROWS, ROWS)]
        for h, (a, b) in enumerate(((0, lat_rows // 2), (lat_rows // 2, lat_rows))):
            w_k = jnp.concatenate([ring[2 * k, a:b], ring[2 * k + 1, a:b]], axis=1)
            d = lax.dot_general(w_k, x_k, (((1,), (1,)), ((), ())), preferred_element_type=F32)
            u[h] = d if k == 0 else u[h] + d
    acc_kv[:lat_rows // 2, :] = u[0]
    acc_kv[lat_rows // 2:lat_rows, :] = u[1]
    acc_kv[lat_rows:, :] = u[1][lat_rows // 2 - ROPE_DIM:, :]
    lat_all = acc_kv[...].T
    ends_rc.start()

    def rotate(z, cos, sin, sel):
        swapped = jnp.where(sel, pltpu.roll(z, LANES - HALF_ROPE, 1), pltpu.roll(z, HALF_ROPE, 1))
        return z * cos + swapped * sin

    own = ds(me * blk, blk)
    for m in range(2):
        lat = lat_all[m * blk:(m + 1) * blk, :KV_LAT]
        inv = lax.rsqrt(jnp.mean(lat * lat, axis=-1, keepdims=True) + NORM_EPS)
        kv_all[m, own, :KV_LAT] = (lat * inv * gain_kv[...].astype(F32).reshape(1, -1)).astype(BF16)
        raw = lat_all[m * blk:(m + 1) * blk, KV_LAT:]
        kv_all[m, own, KV_LAT:] = rotate(raw, trig[0, my_rows(m, core), :], trig[1, my_rows(m, core), :], first_half).astype(BF16)

    def piece(m, dev):
        return kv_all.at[m, ds(dev * blk, blk)]

    def kv_send(i, m, src_dev, role, dev):
        return rcopy(piece(m, src_dev), piece(m, src_dev), kv_ss.at[i], kv_rs.at[role, m], dev)

    def kv_wait(m, src_dev, role):
        rcopy(piece(m, src_dev), piece(m, src_dev), kv_ss.at[0], kv_rs.at[role, m], pair).wait_recv()

    sends = []
    for m in range(2):
        sends.append(kv_send(len(sends), m, me, 2, left))
        sends.append(kv_send(len(sends), m, me, 1, right))
    for m in range(2):
        sends.append(kv_send(len(sends), m, me, 0, pair))
    for c in sends:
        c.start()
    for c in x_rc:
        c.wait_recv()
    my_cols = ds(core * q_cols, q_cols)
    z = [None, None]
    for k in range(n_down):
        for c in qd_copies(k):
            c.wait()
        issue(4 if k == n_down - 1 else 1)
        one, two = qd_refs(k)
        w_k = jnp.concatenate([one[...], two[...]], axis=1)
        for h in range(2):
            d = jnp.dot(x_all[h * q_rows:(h + 1) * q_rows, k * ROWS:(k + 1) * ROWS], w_k, preferred_element_type=F32)
            z[h] = d if k == 0 else z[h] + d
    for h in range(2):
        acc_q[h * q_rows:(h + 1) * q_rows, my_cols] = z[h]
    for i in range(KU_SLOTS):
        ku_copy(i).start(priority=1)
    cq_rc = rcopy(acc_q.at[:, my_cols], acc_q.at[:, my_cols], cq_ss.at[0], cq_rs.at[0], pair)
    cq_rc.start()

    ends_rc.wait_recv()
    for m in range(2):
        positions(m, 1 - core)
    for m in range(2):
        row = lax.broadcasted_iota(jnp.int32, (q_rows, LANES), 0) + chip * q_rows
        start = row.astype(F32) - pos_all[m * q_rows:(m + 1) * q_rows, :]
        for c in range(toks // LANES):
            key = lax.broadcasted_iota(jnp.int32, (q_rows, LANES), 1) + c * LANES
            keep = (key <= row) & (key.astype(F32) >= start)
            cap[m, :, c * LANES:(c + 1) * LANES] = jnp.where(keep, BIG, MASKED)

    cq_rc.wait_recv()
    cq_rc.wait_send()
    for m in range(2):
        for c in range(2):
            lat = acc_q[c * q_rows + m * blk:c * q_rows + (m + 1) * blk, :]
            inv = lax.rsqrt(jnp.mean(lat * lat, axis=-1, keepdims=True) + NORM_EPS)
            cq_all[my_rows(m, c), :] = (lat * inv * gain_q[...].astype(F32).reshape(1, -1)).astype(BF16)

    second = []
    for m in range(2):
        kv_wait(m, left, 1)
        kv_wait(m, right, 2)
    second.append(kv_send(6, 0, left, 3, right))
    second.append(kv_send(7, 1, right, 3, left))
    for m in range(2):
        second.append(kv_send(8 + m, m, left, 4, pair))
        second.append(kv_send(10 + m, m, right, 5, pair))
    for c in second:
        c.start()
    sends += second

    lane2 = lax.broadcasted_iota(jnp.int32, (2 * q_rows, LANES), 1)
    first_half2 = lax.rem(lane2, ROPE_DIM) < HALF_ROPE
    low = lane2 < ROPE_DIM

    f_buf = (acc_q, f_s)
    f_width = QU_HEADS * QK_DIM

    def q_post(t):
        for p in range(QU_HEADS):
            i, base = 2 * t + p // 2, 2 * QK_DIM * (p % 2)
            t0, t1, t2 = (f_buf[t % 2][:, 2 * QK_DIM * p + LANES * n:2 * QK_DIM * p + LANES * (n + 1)] for n in range(3))
            q_s[i, :, base:base + LANES] = t0.astype(BF16)
            q_s[i, :, base + LANES:base + 2 * LANES] = pltpu.roll(jnp.where(low, t2, t1), ROPE_DIM, 1).astype(BF16)
            q_s[i, :, base + 2 * LANES:base + 3 * LANES] = rotate(jnp.where(low, t1, t2), trig[0], trig[1], first_half2).astype(BF16)

    for t in range(n_qu // 2):
        for i in (2 * t, 2 * t + 1):
            for c in qu_copies(i):
                c.wait()
        for i in (2 * t - 2, 2 * t - 1):
            if i >= RING_QU and i + QU_SLOTS < n_qu:
                for c in qu_copies(i + QU_SLOTS):
                    c.start()
        if t == n_qu // 2 - 1:
            third = []
            for m in range(2):
                kv_wait(m, opp, 3)
                third.append(kv_send(12 + m, m, opp, 6, pair))
            for c in third:
                c.start()
            sends += third
        for h in range(2):
            f_buf[t % 2][:, h * f_width:(h + 1) * f_width] = qu_dot(2 * t + h)
        if t > 0:
            q_post(t - 1)
    wo_copy(0).start(priority=1)
    q_post(n_qu // 2 - 1)

    other = 1 - 2 * core
    for m in range(2):
        kv_wait(m, pair, 0)
        kv_wait(m, left + other, 4)
        kv_wait(m, right + other, 5)
        kv_wait(m, opp + other, 6)
    lane3 = lax.broadcasted_iota(jnp.int32, (toks, LANES), 1)
    for m in range(2):
        t = kv_all[m, :, KV_LAT:].astype(F32)
        kr[0, m] = jnp.where(lane3 < ROPE_DIM, t, 0.0).astype(BF16)
        kr[1, m] = jnp.where(lane3 < ROPE_DIM, 0.0, t).astype(BF16)

    exp_scale = QK_DIM ** -0.5 * 1.4426950408889634
    kvs, s_scr, p_scr = (kvs0, kvs1), (s0, s1), (p0, p1)
    o_width = 2 * KU_HEADS * V_DIM

    def o_copy(t):
        cols = ds(t * o_width, o_width)
        return rcopy(o_all.at[core, :, cols], o_all.at[core, :, cols], o_ss.at[t], o_rs.at[t], pair)

    def kv_up(b, i):
        for m in range(2):
            kvs[b][m] = jnp.dot(kv_all[m, :, :KV_LAT], ku[lax.rem(i, KU_SLOTS)], preferred_element_type=F32).astype(BF16)

    def scores(b, t):
        for m in range(2):
            rows = slice(m * q_rows, (m + 1) * q_rows)
            for j in range(KU_HEADS):
                base = 2 * QK_DIM * b
                nope = q_s[t, rows, base + LANES * j:base + LANES * (j + 1)]
                rope = q_s[t, rows, base + 2 * LANES:base + 3 * LANES]
                qc = jnp.concatenate([nope, rope], axis=1)
                kc = jnp.concatenate([kvs[b][m, :, KV_DIM * j:KV_DIM * j + NOPE_DIM], kr[j, m]], axis=1)
                s_scr[b][KU_HEADS * m + j] = lax.dot_general(qc, kc, (((1,), (1,)), ((), ())), preferred_element_type=F32)

    def softmax(b):
        step = 32
        for m in range(2):
            for j in range(KU_HEADS):
                for r in range(q_rows // step):
                    rows = slice(r * step, (r + 1) * step)
                    s = jnp.minimum(s_scr[b][KU_HEADS * m + j, rows, :], cap[m, rows, :])
                    top = jnp.max(s, axis=-1, keepdims=True)
                    e = jnp.exp2((s - top) * exp_scale)
                    inv = 1.0 / jnp.sum(e, axis=-1, keepdims=True)
                    p_scr[b][KU_HEADS * m + j, rows, :] = (e * inv).astype(BF16)

    def values(b, t):
        for m in range(2):
            rows = slice(m * q_rows, (m + 1) * q_rows)
            for j in range(KU_HEADS):
                v = kvs[b][m, :, KV_DIM * j + NOPE_DIM:KV_DIM * (j + 1)]
                o = jnp.dot(p_scr[b][KU_HEADS * m + j], v, preferred_element_type=F32).astype(BF16)
                col = t * o_width + (KU_HEADS * b + j) * V_DIM
                o_all[core, rows, ds(col, V_DIM)] = o

    ku_copy(0).wait()
    kv_up(0, 0)
    scores(0, 0)
    ku_copy(KU_SLOTS).start()
    n_loop = n_ku // 2 - 1

    def at_step(t, carry):
        ku_copy(2 * t + 1).wait()
        ku_copy(2 * t + 2).wait()
        softmax(0)
        kv_up(1, 2 * t + 1)
        values(0, t)
        scores(1, t)
        softmax(1)
        kv_up(0, 2 * t + 2)
        values(1, t)
        scores(0, t + 1)
        for d in (5, 6):
            @pl.when(2 * t + d < n_ku)
            def _():
                ku_copy(2 * t + d).start()
        @pl.when(t + 1 < n_part)
        def _():
            wo_copy(t + 1).start(priority=1)

        o_copy(t).start()
        return carry

    lax.fori_loop(0, n_loop, at_step, 0)
    last = n_loop
    ku_copy(n_ku - 1).wait()
    softmax(0)
    kv_up(1, n_ku - 1)
    values(0, last)
    scores(1, last)
    softmax(1)
    values(1, last)
    o_copy(last).start()

    y_out = (y_one, y_two)

    def y_copies(n):
        slot = n % 2
        cols = ds(core * y_cols + n * COLS, COLS)
        local = [pltpu.make_async_copy(y_st.at[slot, my_rows(m, core)], y_out[m].at[:, cols], y_ls.at[slot, m]) for m in range(2)]
        remote = [rcopy(y_st.at[slot, my_rows(m, 1 - core)], y_out[m].at[:, cols], y_ss.at[slot, m], y_rs.at[n, m], pair) for m in range(2)]
        return local, remote

    def y_wait(n):
        local, remote = y_copies(n)
        for m in range(2):
            local[m].wait()
            remote[m].wait_send()

    def half_dot(g):
        side = lax.rem(core + g, 2)
        w_g = ring[wo_part(g)].reshape(n_wo_k * ROWS, COLS)
        return jnp.dot(o_all[side], w_g, preferred_element_type=F32)

    def y_start(n):
        local, remote = y_copies(n)
        for m in range(2):
            remote[m].start()
            local[m].start()

    wo_copy(0).wait()
    acc = half_dot(0)
    for t in range(n_loop + 1):
        cols = ds(t * o_width, o_width)
        rcopy(o_all.at[1 - core, :, cols], o_all.at[1 - core, :, cols], o_ss.at[t], o_rs.at[t], pair).wait_recv()
    wo_copy(1).wait()
    acc = acc + half_dot(1)
    for n in range(1, n_wo_n + 1):
        if n < n_wo_n:
            for g in (2 * n, 2 * n + 1):
                wo_copy(g).wait()
        if n >= 2:
            y_start(n - 2)
        if n >= 3:
            y_wait(n - 3)
        for g in (2 * n - 2 + n_part, 2 * n - 1 + n_part):
            if g < n_wo:
                wo_copy(g).start()
        y_st[(n - 1) % 2] = acc.astype(BF16)
        if n < n_wo_n:
            acc = half_dot(2 * n) + half_dot(2 * n + 1)
    y_start(n_wo_n - 1)
    y_wait(n_wo_n - 2)
    y_wait(n_wo_n - 1)
    for n in range(n_wo_n):
        cols = ds((1 - core) * y_cols + n * COLS, COLS)
        for m in range(2):
            rcopy(y_st.at[0, my_rows(m, core)], y_out[m].at[:, cols], y_ss.at[0, m], y_rs.at[n, m], pair).wait_recv()
    for c in x_rc + [ends_rc]:
        c.wait_send()
    for c in sends:
        c.wait_send()
    for t in range(n_loop + 1):
        o_copy(t).wait_send()


def mla(n_sp, x_one, x_two, pos_one, pos_two, freq, w_qd, gain_q, w_qu, w_kvd, gain_kv, w_kvu, w_out):
    blk, d_model = x_one.shape
    heads = w_out.shape[0] * w_out.shape[1] // V_DIM
    toks = n_sp * blk
    q_rows = 2 * blk
    n_down = d_model // ROWS
    n_qu = heads // 2 // QU_HEADS
    n_ku = heads // 2 // KU_HEADS
    n_wo_n = d_model // 2 // COLS
    hbm = pl.BlockSpec(memory_space=pl.ANY)
    vmem = pl.BlockSpec(memory_space=pltpu.VMEM)
    dma = pltpu.SemaphoreType.DMA
    units = 2 * KU_HEADS
    return pl.pallas_call(
        functools.partial(body, n_sp, heads, d_model, blk),
        out_shape=[jax.ShapeDtypeStruct((blk, d_model), BF16)] * 2,
        in_specs=[hbm, hbm, hbm, hbm, vmem, hbm, vmem, hbm, hbm, vmem, hbm, hbm],
        out_specs=[hbm, hbm],
        scratch_shapes=[
            pltpu.VMEM((2 * q_rows, d_model), BF16),
            pltpu.SMEM((2, blk), jnp.int32),
            pltpu.VMEM((2, 4, 8, LANES), F32),
            pltpu.VMEM((2 * q_rows, LANES), F32),
            pltpu.VMEM((2, 2 * q_rows, LANES), F32),
            pltpu.VMEM((RING, ROWS, COLS), BF16),
            pltpu.VMEM((QU_SLOTS, Q_LAT, QU_HEADS * QK_DIM), BF16),
            pltpu.VMEM((KU_SLOTS, KV_LAT, KU_HEADS * KV_DIM), BF16),
            pltpu.VMEM((KV_LAT + 2 * ROPE_DIM, 2 * blk), F32),
            pltpu.VMEM((2 * q_rows, Q_LAT), F32),
            pltpu.VMEM((2, toks, KVW), BF16),
            pltpu.VMEM((2 * q_rows, Q_LAT), BF16),
            pltpu.VMEM((2, q_rows, toks), F32),
            pltpu.VMEM((2, 2, toks, LANES), BF16),
            pltpu.VMEM((n_qu, 2 * q_rows, QU_HEADS * QK_DIM), BF16),
            pltpu.VMEM((2 * q_rows, 2 * QU_HEADS * QK_DIM), F32),
            pltpu.VMEM((2, toks, KU_HEADS * KV_DIM), BF16),
            pltpu.VMEM((2, toks, KU_HEADS * KV_DIM), BF16),
            pltpu.VMEM((units, q_rows, toks), F32),
            pltpu.VMEM((units, q_rows, toks), F32),
            pltpu.VMEM((units, q_rows, toks), BF16),
            pltpu.VMEM((units, q_rows, toks), BF16),
            pltpu.VMEM((2, 2 * q_rows, heads // 2 * V_DIM), BF16),
            pltpu.VMEM((2, 2 * q_rows, COLS), BF16),
            dma((2,)), dma((2,)), dma((2,)), dma((2,)), dma((1,)), dma((1,)),
            dma((d_model // COLS,)), dma((n_down, 2)), dma((n_qu, 4)), dma((KU_SLOTS,)), dma((WO_RING,)),
            dma((14,)), dma((7, 2)),
            dma((1,)), dma((1,)),
            dma((n_ku // 2,)), dma((n_ku // 2,)),
            dma((2, 2)), dma((2, 2)), dma((n_wo_n, 2)),
        ],
        compiler_params=pltpu.CompilerParams(
            collective_id=0, has_side_effects=True, vmem_limit_bytes=67043328),
        name="mla",
    )(x_one, x_two, pos_one, pos_two, freq, w_qd, gain_q, w_qu, w_kvd, gain_kv, w_kvu, w_out)


PASS_PARTS = 4


def pass_body(one_in, two_in, one_out, two_out, buf, in_sem, out_sem):
    blk, d_model = one_in.shape
    width = d_model // PASS_PARTS
    moves = []
    for n in range(PASS_PARTS):
        cols = pl.ds(n * width, width)
        for m, (src, dst) in enumerate(((one_in, one_out), (two_in, two_out))):
            moves.append((pltpu.make_async_copy(src.at[:, cols], buf.at[m, n], in_sem.at[m, n]),
                          pltpu.make_async_copy(buf.at[m, n], dst.at[:, cols], out_sem.at[m, n])))
    for load, _ in moves:
        load.start()
    for load, store in moves:
        load.wait()
        store.start()
    for _, store in moves:
        store.wait()


def pass_on(y_one, y_two):
    blk, d_model = y_one.shape
    hbm = pl.BlockSpec(memory_space=pl.ANY)
    dma = pltpu.SemaphoreType.DMA
    return pl.pallas_call(
        pass_body,
        out_shape=[jax.ShapeDtypeStruct(y_one.shape, y_one.dtype)] * 2,
        in_specs=[hbm, hbm], out_specs=[hbm, hbm],
        scratch_shapes=[pltpu.VMEM((2, PASS_PARTS, blk, d_model // PASS_PARTS), BF16),
                        dma((2, PASS_PARTS)), dma((2, PASS_PARTS))],
        compiler_params=pltpu.CompilerParams(vmem_limit_bytes=67043328),
        name="pass_on",
    )(y_one, y_two)


def solution(mesh):
    tok_spec = P(('dp', 'sp'), None)
    idx_spec = P(('dp', 'sp'))
    n_sp = mesh.shape['sp']
    freq = ROPE_BASE ** (-(np.arange(LANES) % HALF_ROPE).astype(np.float64) / HALF_ROPE)
    freq = freq.astype(np.float32)[None, :]

    def local_body(x_one, seg_one, pos_one, x_two, seg_two, pos_two, w_qdown, gain_q, w_qup, w_kvdown, gain_kv, w_kvup, w_out):
        y_one, y_two = mla(n_sp, x_one, x_two, pos_one, pos_two, jnp.asarray(freq), w_qdown, gain_q, w_qup, w_kvdown.T, gain_kv, w_kvup, w_out.reshape(-1, ROWS, w_out.shape[1]))
        return pass_on(y_one, y_two)

    return jax.shard_map(local_body, mesh=mesh, in_specs=(tok_spec, idx_spec, idx_spec, tok_spec, idx_spec, idx_spec) + (P(),) * 7, out_specs=(tok_spec, tok_spec), check_vma=False)
```
